256 devices in a mesh: view: 8 (over x, core), gauss: 32 (over y, z).
Axes of the slice: x: 4, y: 4, z: 8, core: 2. Of those that a mesh axis runs over, the one named last changes fastest.
Arguments:
- means: float32 [3, 524288], P(None, 'gauss'), may hold values from -1 to 1
- scales: float32 [3, 524288], P(None, 'gauss'), may hold values from 0.05 to 0.6
- quats: float32 [4, 524288], P(None, 'gauss'), may hold values from -6 to 6
- attrs: float32 [49, 524288], P(None, 'gauss'), may hold values from -6 to 6
- grad_screen: float32 [32, 2, 524288], P('view', None, 'gauss'), may hold values from -6 to 6
- visible: int32 [32, 524288], P('view', 'gauss'), may hold values 0 or 1
- clone_mask: int32 [524288], P('gauss'), may hold values from 0 to 1, as said below
- rotation: float32 [32, 3, 3], P('view'), may hold values from -3.5 to 3.5
- shift: float32 [32, 3], P('view'), may hold values from 2 to 5
- focal: float32 [32], P('view'), may hold values from 1 to 4
Outputs:
- peak_stats: float32 [2, 524288], P(None, 'gauss')
- clones: float32 [61, 524288], P(None, 'gauss')
- clone_total: int32 [], replicated
The draws below stay inside these ranges and needn't reach their ends.
Inputs may be any that keep to these rules, and one draw needn't show every extreme that they name: `clone_mask`: in every draw some shard of 16384 consecutive Gaussians has all of them marked.
All inputs are finite; a program needn't handle non-finite values. No bound on the sum of `visible` on one device may be relied on, other than what follows from the above.
Results may differ from the reference program's by a relative error of at most 0.0003.
Values sent between devices are 32-bit elements; how exact they have to be, the bound alone decides.
A program may use at most 128 MiB of HBM per device.

```python
import math
import jax
import jax.numpy as jnp
from jax import lax

G_DEV = 16384
ATTR = 49
GAUSSIANS = 524288
VIEWS = 32
N_GAUSS = 32


def draw_clone_mask(key, part):
    shards = GAUSSIANS // G_DEV
    most = G_DEV // 128 * 128
    first, second, third = jax.random.split(key, 3)
    raw = jax.random.randint(first, (shards,), 0, most + 1)
    counts = raw * raw // most
    chosen = jax.random.randint(second, (), 0, shards)
    counts = jnp.where(jnp.arange(shards) == chosen, most, counts)
    keys = jax.random.split(third, shards)
    orders = jax.vmap(lambda k: jax.random.permutation(k, G_DEV))(keys)
    return (orders < counts[:, None]).astype(jnp.int32).reshape(-1)


def with_ends(result, stream_key, least, high):
    longest = result.shape.index(max(result.shape))
    spots = []
    for shift in (0, 1):
        where = [jax.random.randint(jax.random.fold_in(stream_key, axis), (), 0, length) for axis, length in enumerate(result.shape)]
        where[longest] = (where[longest] + shift) % result.shape[longest]
        spots.append(tuple(where))
    return result.at[spots[0]].set(least).at[spots[1]].set(high)


def level_of(own_key, extent, pieces, smallest, top_value):
    def one(dim, shards_of):
        steps = jax.random.uniform(jax.random.fold_in(jax.random.fold_in(own_key, 6), dim), (shards_of,), jnp.float32, smallest / len(pieces), top_value / len(pieces))
        return jnp.repeat(jnp.exp(steps), extent[dim] // shards_of).reshape((-1,) + (1,) * (len(extent) - dim - 1))

    loudness = one(*pieces[0])
    for cut in pieces[1:]:
        loudness = loudness * one(*cut)
    return loudness


def centred(own_key, dims, deviation, reach, cuts=(), dtype=jnp.bfloat16):
    result = deviation * jax.random.normal(own_key, dims, jnp.float32)
    if cuts:
        result = result * level_of(own_key, dims, cuts, -0.22, 0.18)
    return jnp.clip(result, -reach, reach).astype(dtype)


def setup_inputs(seed: int = 0) -> dict:
    arg_keys = jax.random.split(jax.random.key(seed), 11)
    return {
        "means": jnp.clip(jax.random.uniform(arg_keys[0], (3, GAUSSIANS), jnp.float32, -1.0, 1.0) * level_of(arg_keys[0], (3, GAUSSIANS), ((1, 32),), -0.4, 0.0), -1.0, 1.0),
        "scales": jnp.clip(jnp.exp(math.log(0.6) - 2.4849067 * jax.random.uniform(arg_keys[1], (3, GAUSSIANS), jnp.float32) ** level_of(arg_keys[1], (3, GAUSSIANS), ((1, 32),), -0.2, 0.2)), 0.05, 0.6),
        "quats": centred(arg_keys[2], (4, GAUSSIANS), 1.0, 6.0, ((1, 32),), jnp.float32),
        "attrs": centred(arg_keys[3], (ATTR, GAUSSIANS), 1.0, 6.0, ((1, 32),), jnp.float32),
        "grad_screen": centred(arg_keys[4], (VIEWS, 2, GAUSSIANS), 1.0, 6.0, ((0, 8), (2, 32)), jnp.float32),
        "visible": with_ends((jax.random.randint(arg_keys[5], (VIEWS, GAUSSIANS), 0, 4) < 3).astype(jnp.int32), jax.random.fold_in(arg_keys[5], 1), 0, 1),
        "clone_mask": draw_clone_mask(jax.random.fold_in(arg_keys[10], 71), 0),
        "rotation": centred(arg_keys[7], (VIEWS, 3, 3), 3 ** -0.5, 3.5, ((0, 8),), jnp.float32),
        "shift": jnp.clip(2.0 + 3.0 * jax.random.uniform(arg_keys[8], (VIEWS, 3), jnp.float32) ** level_of(arg_keys[8], (VIEWS, 3), ((0, 8),), -0.2, 0.2), 2.0, 5.0),
        "focal": jnp.clip(jnp.exp(math.log(4.0) - 1.3862944 * jax.random.uniform(arg_keys[9], (VIEWS,), jnp.float32) ** level_of(arg_keys[9], (VIEWS,), ((0, 8),), -0.2, 0.2)), 1.0, 4.0),
    }


def quat_factor(scales, quats):
    inv = 1.0 / jnp.sqrt(lax.optimization_barrier(jnp.sum(quats * quats, axis=0)) + 0.25)
    w, x, y, z = (quats[0] * inv, quats[1] * inv, quats[2] * inv, quats[3] * inv)
    rq = [[1 - 2 * (y * y + z * z), 2 * (x * y - w * z), 2 * (x * z + w * y)], [2 * (x * y + w * z), 1 - 2 * (x * x + z * z), 2 * (y * z - w * x)], [2 * (x * z - w * y), 2 * (y * z + w * x), 1 - 2 * (x * x + y * y)]]
    return [[rq[i][j] * scales[j] for j in range(3)] for i in range(3)]

def view_stats(means, factor, grad, seen, rot, trans, focal_v):
    point = [rot[i, 0] * means[0] + rot[i, 1] * means[1] + rot[i, 2] * means[2] + trans[i] for i in range(3)]
    depth = jnp.maximum(point[2], 1.0)
    j00 = focal_v / depth
    j02 = -focal_v * point[0] / (depth * depth)
    j12 = -focal_v * point[1] / (depth * depth)
    first = [j00 * rot[0, j] + j02 * rot[2, j] for j in range(3)]
    second = [j00 * rot[1, j] + j12 * rot[2, j] for j in range(3)]
    prow = [sum((first[j] * factor[j][k] for j in range(3))) for k in range(3)]
    qrow = [sum((second[j] * factor[j][k] for j in range(3))) for k in range(3)]
    a_val = prow[0] ** 2 + prow[1] ** 2 + prow[2] ** 2 + 0.3
    c_val = qrow[0] ** 2 + qrow[1] ** 2 + qrow[2] ** 2 + 0.3
    b_val = prow[0] * qrow[0] + prow[1] * qrow[1] + prow[2] * qrow[2]
    half = 0.5 * (a_val - c_val)
    lam = 0.5 * (a_val + c_val) + jnp.sqrt(half * half + b_val * b_val + 0.01)
    seenf = seen.astype(jnp.float32)
    radius = 3.0 * jnp.sqrt(lam) * seenf
    gnorm = jnp.sqrt(grad[0] * grad[0] + grad[1] * grad[1]) * seenf
    return (gnorm, radius)

def reference(means, scales, quats, attrs, grad_screen, visible, clone_mask, rotation, shift, focal):
    factor = quat_factor(scales, quats)
    gmax = jnp.zeros(means.shape[1], jnp.float32)
    rmax = jnp.zeros(means.shape[1], jnp.float32)
    for v in range(grad_screen.shape[0]):
        gnorm, radius = view_stats(means, factor, grad_screen[v], visible[v], rotation[v], shift[v], focal[v])
        gmax = jnp.maximum(gmax, gnorm)
        rmax = jnp.maximum(rmax, radius)
    peak = jnp.stack([gmax, rmax])
    rows = jnp.concatenate([means, scales, quats, attrs, peak], axis=0)
    shards = N_GAUSS
    cap = G_DEV // 128 * 128
    marks = clone_mask.reshape(shards, G_DEV)
    rank = jnp.cumsum(marks, axis=1).astype(jnp.int32) - 1
    counts = lax.optimization_barrier(jnp.sum(marks, axis=1)).astype(jnp.int32)
    blocks = (counts + 127) // 128
    offset = (jnp.cumsum(blocks) - blocks).astype(jnp.int32)
    block = offset[:, None] + rank // 128
    column = block % shards * cap + block // shards * 128 + rank % 128
    column = jnp.where(marks == 1, column, shards * cap).reshape(-1).astype(jnp.int32)
    clones = jnp.zeros((rows.shape[0], shards * cap), jnp.float32).at[:, column].set(rows, mode='drop')
    total = jnp.sum(clone_mask).astype(jnp.int32)
    return (peak, clones, total)
```

```python
import functools

import jax
import jax.numpy as jnp
from jax import lax
from jax.experimental import pallas as pl
from jax.experimental.pallas import tpu as pltpu
from jax.sharding import PartitionSpec as P

G = 16384
ROWS = 61
BLK = 128
CAP = G // BLK
NV = 8
NG = 32
PER = CAP // NG
MESH = pl.DeviceIdType.MESH
VMEM = pl.BlockSpec(memory_space=pltpu.VMEM)
SMEM = pl.BlockSpec(memory_space=pltpu.SMEM)
ANY = pl.BlockSpec(memory_space=pl.ANY)


def stats_kernel(means, scales, quats, grad, seen, mask, rot, trans, focal, out, count):
    views = grad.shape[0]

    def step(c, _):
        s = pl.ds(pl.multiple_of(c * 1024, 1024), 1024)

        def row(ref, *at):
            return ref[at[:-1] + (slice(at[-1], at[-1] + 1), s)].reshape(8, 128)

        m = [row(means, i) for i in range(3)]
        sc = [row(scales, i) for i in range(3)]
        q = [row(quats, i) for i in range(4)]
        inv = 1.0 / jnp.sqrt(q[0] * q[0] + q[1] * q[1] + q[2] * q[2] + q[3] * q[3] + 0.25)
        w, x, y, z = (t * inv for t in q)
        rq = [
            [1 - 2 * (y * y + z * z), 2 * (x * y - w * z), 2 * (x * z + w * y)],
            [2 * (x * y + w * z), 1 - 2 * (x * x + z * z), 2 * (y * z - w * x)],
            [2 * (x * z - w * y), 2 * (y * z + w * x), 1 - 2 * (x * x + y * y)],
        ]
        factor = [[rq[i][j] * sc[j] for j in range(3)] for i in range(3)]
        gbest = jnp.zeros((8, 128), jnp.float32)
        lbest = jnp.zeros((8, 128), jnp.float32)
        for v in range(views):
            r = [[rot[v, i, j] for j in range(3)] for i in range(3)]
            p = [r[i][0] * m[0] + r[i][1] * m[1] + r[i][2] * m[2] + trans[v, i] for i in range(3)]
            near = 1.0 / jnp.maximum(p[2], 1.0)
            f = focal[v]
            j00 = f * near
            j02 = -j00 * p[0] * near
            j12 = -j00 * p[1] * near
            first = [j00 * r[0][j] + j02 * r[2][j] for j in range(3)]
            second = [j00 * r[1][j] + j12 * r[2][j] for j in range(3)]
            pr = [sum(first[j] * factor[j][k] for j in range(3)) for k in range(3)]
            qr = [sum(second[j] * factor[j][k] for j in range(3)) for k in range(3)]
            a = pr[0] * pr[0] + pr[1] * pr[1] + pr[2] * pr[2] + 0.3
            cc = qr[0] * qr[0] + qr[1] * qr[1] + qr[2] * qr[2] + 0.3
            b = pr[0] * qr[0] + pr[1] * qr[1] + pr[2] * qr[2]
            half = 0.5 * (a - cc)
            lam = 0.5 * (a + cc) + jnp.sqrt(half * half + b * b + 0.01)
            on = row(seen, v) > 0
            g0, g1 = row(grad, v, 0), row(grad, v, 1)
            gbest = jnp.maximum(gbest, jnp.where(on, g0 * g0 + g1 * g1, 0.0))
            lbest = jnp.maximum(lbest, jnp.where(on, lam, 0.0))
        part, at = c // 2, pl.multiple_of((c % 2) * 8, 8)
        out[part, 0, pl.ds(at, 8), :] = gbest
        out[part, 1, pl.ds(at, 8), :] = lbest
        return 0

    lax.fori_loop(0, 16, step, 0)
    columns = jnp.sum(mask[...].astype(jnp.float32), axis=0, keepdims=True)
    total = jnp.sum(columns, axis=1, keepdims=True)
    count[...] = jnp.broadcast_to(total, (8, 128)).astype(jnp.int32)


def peaks_kernel(part, count, best, counts, taken, merged, s1, r1, s2, r2, s3, r3):
    v, g = lax.axis_index("view"), lax.axis_index("gauss")
    barrier = pltpu.get_barrier_semaphore()

    def hello_v(i, _):
        pl.semaphore_signal(barrier, inc=1, device_id={"view": (v + i) % NV}, device_id_type=MESH)
        return 0

    def hello_g(i, _):
        pl.semaphore_signal(barrier, inc=1, device_id={"gauss": (g + i) % NG}, device_id_type=MESH)
        return 0

    lax.fori_loop(1, NV, hello_v, 0)
    lax.fori_loop(1, NG, hello_g, 0)
    pl.semaphore_wait(barrier, NV - 1 + NG - 1)

    def scatter(i, slot):
        peer = (v + i) % NV
        return pltpu.make_async_remote_copy(
            part.at[peer], taken.at[slot], s1.at[i], r1.at[slot], device_id={"view": peer}, device_id_type=MESH
        )

    def spread(i, slot):
        peer = (v + i) % NV
        return pltpu.make_async_remote_copy(
            merged, best.at[slot], s2.at[i], r2.at[slot], device_id={"view": peer}, device_id_type=MESH
        )

    def tell(i, slot):
        peer = (g + i) % NG
        return pltpu.make_async_remote_copy(
            count, counts.at[slot], s3.at[i], r3.at[slot], device_id={"gauss": peer}, device_id_type=MESH
        )

    def each(n, do):
        def one(i, _):
            do(i)
            return 0

        lax.fori_loop(1, n, one, 0)

    each(NV, lambda i: scatter(i, v).start())
    each(NG, lambda i: tell(i, g).start())
    counts[g] = count[...]
    each(NV, lambda i: scatter(i, (v + i) % NV).wait_recv())

    top = part[v]

    def merge(i, top):
        return jnp.maximum(top, taken[(v + i) % NV])

    top = lax.fori_loop(1, NV, merge, top)
    merged[...] = top
    best[v] = top
    each(NV, lambda i: spread(i, v).start())
    each(NV, lambda i: spread(i, (v + i) % NV).wait_recv())
    each(NG, lambda i: tell(i, (g + i) % NG).wait_recv())
    each(NV, lambda i: scatter(i, v).wait_send())
    each(NV, lambda i: spread(i, v).wait_send())
    each(NG, lambda i: tell(i, g).wait_send())


def pack_kernel(mask, counts, best, means, scales, quats, attrs, out, table, peak, xa, xb, x, picks, tab, stab, sem):
    v, g = lax.axis_index("view"), lax.axis_index("gauss")
    a_at = pl.multiple_of(jnp.clip(v - 2, 0, 5) * 8, 8)
    b_at = pl.multiple_of(jnp.clip(v - 1, 0, 5) * 8, 8)
    load_a = pltpu.make_async_copy(attrs.at[pl.ds(a_at, 8), :], xa, sem.at[0])
    load_b = pltpu.make_async_copy(attrs.at[pl.ds(b_at, 8), :], xb, sem.at[1])
    load_c = pltpu.make_async_copy(attrs.at[48:49, :], xb.at[0:1, :], sem.at[1])
    load_a.start()

    @pl.when(v < 7)
    def _():
        load_b.start()

    @pl.when(v == 7)
    def _():
        load_c.start()

    sub = lax.broadcasted_iota(jnp.int32, (8, 128), 0)
    lane = lax.broadcasted_iota(jnp.int32, (8, 128), 1)
    k = lane * NG + g
    off = jnp.zeros((8, 128), jnp.int32)
    mine = jnp.zeros((8, 128), jnp.int32)
    total = jnp.zeros((8, 128), jnp.int32)
    source = jnp.full((8, 128), CAP, jnp.int32)
    for s in range(NG):
        n = counts[s]
        blocks = (n + (BLK - 1)) >> 7
        mine = mine + jnp.where(s < g, blocks, 0)
        inside = (k >= off) & (k < off + blocks)
        source = jnp.where(inside, s * PER + ((k - off) >> 5), source)
        off = off + blocks
        total = total + n
    slots = (off + (NG - 1)) >> 5
    table[...] = jnp.where(sub == 0, source, jnp.where(sub == 1, total, slots))

    marks = mask[...].astype(jnp.float32).astype(jnp.bfloat16)
    i0 = lax.broadcasted_iota(jnp.int32, (128, 128), 0)
    i1 = lax.broadcasted_iota(jnp.int32, (128, 128), 1)
    upto = (i0 <= i1).astype(jnp.float32).astype(jnp.bfloat16)
    before = (i0 < i1).astype(jnp.float32).astype(jnp.bfloat16)
    run = jnp.dot(marks, upto, preferred_element_type=jnp.float32).astype(jnp.int32)
    per_row = lax.dot_general(
        jnp.ones((8, 128), jnp.bfloat16), marks, (((1,), (1,)), ((), ())), preferred_element_type=jnp.float32
    )
    base = jnp.dot(per_row.astype(jnp.bfloat16), before, preferred_element_type=jnp.float32)
    end = (base + per_row).astype(jnp.int32)
    tab[...] = jnp.where(sub == 0, base.astype(jnp.int32), jnp.where(sub == 1, end, mine))
    to_smem = pltpu.make_async_copy(tab, stab, sem.at[2])
    to_smem.start()

    e = jnp.where(mask[...] > 0, i1 + ((i1 - run + 1) << 8), 0)
    for bit in range(7):
        far = pltpu.roll(e, 128 - (1 << bit), axis=1)
        comes = (far & (256 << bit)) != 0
        goes = (e & (256 << bit)) != 0
        e = jnp.where(comes, far, jnp.where(goes, 0, e))
    picks[...] = e & 255

    def roots(c, _):
        s = pl.ds(pl.multiple_of(c * 1024, 1024), 1024)
        part, at = c // 2, pl.multiple_of((c % 2) * 8, 8)
        peak[0:1, s] = jnp.sqrt(best[part, 0, pl.ds(at, 8), :]).reshape(1, 1024)
        peak[1:2, s] = (3.0 * jnp.sqrt(best[part, 1, pl.ds(at, 8), :])).reshape(1, 1024)
        return 0

    lax.fori_loop(0, 16, roots, 0)

    load_a.wait()

    @pl.when(v < 7)
    def _():
        load_b.wait()

    @pl.when(v == 7)
    def _():
        load_c.wait()

    @pl.when(v == 0)
    def _():
        x[0:3, :] = means[...]
        x[3:6, :] = scales[...]
        x[6:8, :] = quats[0:2, :]

    @pl.when(v == 1)
    def _():
        x[0:2, :] = quats[2:4, :]
        x[2:8, :] = xb[0:6, :]

    @pl.when((v > 1) & (v < 7))
    def _():
        x[0:2, :] = xa[6:8, :]
        x[2:8, :] = xb[0:6, :]

    @pl.when(v == 7)
    def _():
        x[0:2, :] = xa[6:8, :]
        x[2:3, :] = xb[0:1, :]
        x[3:5, :] = peak[...]
        x[5:8, :] = jnp.zeros((3, G), jnp.float32)

    to_smem.wait()
    shift = stab[2, 0]

    def home(block):
        return ((shift + block) & (NG - 1)) * PER + (block >> 5)

    def pack(c, carry):
        start, stop = stab[0, c], stab[1, c]
        block, r = start >> 7, start & 127
        tile = x[:, pl.ds(pl.multiple_of(c * 128, 128), 128)]
        pick = jnp.broadcast_to(picks[pl.ds(c, 1), :], (8, 128))
        got = jnp.take_along_axis(tile, pick, axis=1, mode="promise_in_bounds")
        got = pltpu.roll(got, r, axis=1)
        live = ((lane - r) & 127) < (stop - start)
        now = jnp.where(live & (lane >= r), got, carry)
        later = jnp.where(live & (lane < r), got, 0.0)
        out[home(block)] = now
        return jnp.where((stop >> 7) > block, later, now)

    carry = lax.fori_loop(0, 128, pack, jnp.zeros((8, 128), jnp.float32), unroll=4)
    last = stab[1, 127]

    @pl.when(last < G)
    def _():
        out[home(last >> 7)] = carry


def move_kernel(tiles, table, out, taken, placed, s1, r1, s2, r2, s3, r3, own):
    v, g = lax.axis_index("view"), lax.axis_index("gauss")
    core, chip = v % 2, v // 2
    barrier = pltpu.get_barrier_semaphore()

    def each(lo, n, do):
        def one(i, _):
            do(i)
            return 0

        lax.fori_loop(lo, n, one, 0)

    each(1, NV, lambda i: pl.semaphore_signal(barrier, inc=1, device_id={"view": (v + i) % NV}, device_id_type=MESH))
    each(1, NG, lambda i: pl.semaphore_signal(barrier, inc=1, device_id={"gauss": (g + i) % NG}, device_id_type=MESH))
    pl.semaphore_wait(barrier, NV - 1 + NG - 1)

    def send(i, slot):
        peer = (g + i) % NG
        return pltpu.make_async_remote_copy(
            tiles.at[pl.ds(peer * PER, PER)],
            taken.at[pl.ds(slot * PER, PER)],
            s1.at[i],
            r1.at[slot],
            device_id={"gauss": peer},
            device_id_type=MESH,
        )

    each(1, NG, lambda i: send(i, g).start())
    keep = pltpu.make_async_copy(tiles.at[pl.ds(g * PER, PER)], taken.at[pl.ds(g * PER, PER)], own.at[0])
    keep.start()
    taken[CAP] = jnp.zeros((8, 128), jnp.float32)
    keep.wait()
    each(1, NG, lambda i: send(i, (g + i) % NG).wait_recv())

    def place(q, _):
        placed[q] = taken[table[0, q]]
        return 0

    lax.fori_loop(0, CAP, place, 0)

    def away(i, slot):
        peer = ((chip + i) % 4) * 2 + core
        return pltpu.make_async_remote_copy(
            placed, out.at[slot], s2.at[i], r2.at[slot], device_id={"view": peer}, device_id_type=MESH
        )

    def beside(i, slot):
        src = placed if i is None else out.at[slot]
        at = 0 if i is None else i
        return pltpu.make_async_remote_copy(
            src, out.at[slot], s3.at[at], r3.at[slot], device_id={"view": chip * 2 + 1 - core}, device_id_type=MESH
        )

    each(1, 4, lambda i: away(i, v).start())
    beside(None, v).start()
    mine = pltpu.make_async_copy(placed, out.at[v], own.at[0])
    mine.start()

    def relay(i):
        slot = ((chip + i) % 4) * 2 + core
        away(i, slot).wait_recv()
        beside(i, slot).start()

    each(1, 4, relay)
    mine.wait()
    beside(None, chip * 2 + 1 - core).wait_recv()
    each(1, 4, lambda i: beside(i, ((chip + i) % 4) * 2 + 1 - core).wait_recv())
    each(1, 4, lambda i: away(i, v).wait_send())
    beside(None, v).wait_send()
    each(1, 4, lambda i: beside(i, ((chip + i) % 4) * 2 + core).wait_send())
    each(1, NG, lambda i: send(i, g).wait_send())


HALF = 64


def lay_kernel(slots, tiles, out):
    h = pl.program_id(1)
    for q in range(HALF):
        out[:, q * BLK : (q + 1) * BLK] = jnp.where(h * HALF + q < slots[0], tiles[0, q], 0.0)


def body(means, scales, quats, attrs, grad_screen, visible, clone_mask, rotation, shift, focal):
    f32, i32 = jnp.float32, jnp.int32
    mask = clone_mask.reshape(128, 128)
    part, count = pl.pallas_call(
        stats_kernel,
        in_specs=[VMEM] * 6 + [SMEM] * 3,
        out_specs=(VMEM, VMEM),
        out_shape=(jax.ShapeDtypeStruct((NV, 2, 16, 128), f32), jax.ShapeDtypeStruct((8, 128), i32)),
        name="stats",
    )(means, scales, quats, grad_screen, visible, mask, rotation, shift, focal)

    dma = pltpu.SemaphoreType.DMA
    best, counts = pl.pallas_call(
        peaks_kernel,
        in_specs=[VMEM] * 2,
        out_specs=(VMEM, VMEM),
        out_shape=(jax.ShapeDtypeStruct((NV, 2, 16, 128), f32), jax.ShapeDtypeStruct((NG, 8, 128), i32)),
        scratch_shapes=[
            pltpu.VMEM((NV, 2, 16, 128), f32),
            pltpu.VMEM((2, 16, 128), f32),
            dma((NV,)),
            dma((NV,)),
            dma((NV,)),
            dma((NV,)),
            dma((NG,)),
            dma((NG,)),
        ],
        compiler_params=pltpu.CompilerParams(collective_id=0, has_side_effects=True),
        name="peaks",
    )(part, count)

    tiles, table, peak = pl.pallas_call(
        pack_kernel,
        in_specs=[VMEM] * 6 + [ANY],
        out_specs=(VMEM, VMEM, VMEM),
        out_shape=(
            jax.ShapeDtypeStruct((CAP, 8, 128), f32),
            jax.ShapeDtypeStruct((8, 128), i32),
            jax.ShapeDtypeStruct((2, G), f32),
        ),
        scratch_shapes=[
            pltpu.VMEM((8, G), f32),
            pltpu.VMEM((8, G), f32),
            pltpu.VMEM((8, G), f32),
            pltpu.VMEM((128, 128), i32),
            pltpu.VMEM((8, 128), i32),
            pltpu.SMEM((8, 128), i32),
            dma((3,)),
        ],
        name="pack",
    )(mask, counts, best, means, scales, quats, attrs)

    gathered = pl.pallas_call(
        move_kernel,
        in_specs=[VMEM, SMEM],
        out_specs=ANY,
        out_shape=jax.ShapeDtypeStruct((NV, CAP, 8, 128), f32),
        scratch_shapes=[
            pltpu.VMEM((CAP + 1, 8, 128), f32),
            pltpu.VMEM((CAP, 8, 128), f32),
            dma((NG,)),
            dma((NG,)),
            dma((4,)),
            dma((NV,)),
            dma((4,)),
            dma((NV,)),
            dma((1,)),
        ],
        compiler_params=pltpu.CompilerParams(collective_id=1, has_side_effects=True),
        name="move",
    )(tiles, table)

    slots = table[2, :1]
    clones = pl.pallas_call(
        lay_kernel,
        grid_spec=pltpu.PrefetchScalarGridSpec(
            num_scalar_prefetch=1,
            grid=(NV, CAP // HALF),
            in_specs=[
                pl.BlockSpec(
                    (1, HALF, 8, 128), lambda r, h, n: (r, jnp.minimum(h, (jnp.maximum(n[0], 1) - 1) // HALF), 0, 0)
                )
            ],
            out_specs=pl.BlockSpec((8, HALF * BLK), lambda r, h, n: (r, h)),
        ),
        out_shape=jax.ShapeDtypeStruct((ROWS, G), f32),
        name="lay",
    )(slots, gathered)
    return (peak, clones, table[1, 0])


def solution(mesh):
    return jax.shard_map(
        body,
        mesh=mesh,
        in_specs=(
            P(None, "gauss"),
            P(None, "gauss"),
            P(None, "gauss"),
            P(None, "gauss"),
            P("view", None, "gauss"),
            P("view", "gauss"),
            P("gauss"),
            P("view", None, None),
            P("view", None),
            P("view"),
        ),
        out_specs=(P(None, "gauss"), P(None, "gauss"), P()),
        check_vma=False,
    )
```

```python
import jax
import jax.numpy as jnp
from jax import lax
from jax.experimental import pallas as pl
from jax.experimental.pallas import tpu as pltpu
from jax.sharding import PartitionSpec as P

G = 16384
ROWS = 61
BLK = 128
CAP = G // BLK
NV = 8
NG = 32
PER = CAP // NG
PAIR = PER * BLK
CHUNKS = 8
WIDE = G // CHUNKS
MESH = pl.DeviceIdType.MESH
VMEM = pl.BlockSpec(memory_space=pltpu.VMEM)
SMEM = pl.BlockSpec(memory_space=pltpu.SMEM)
ANY = pl.BlockSpec(memory_space=pl.ANY)


def each(lo, n, do):
    def one(i, _):
        do(i)
        return 0

    lax.fori_loop(lo, n, one, 0)


def front_kernel(
    mask, means, scales, quats, grad, seen, rot, trans, focal, attrs,
    part, packed, tiles, count,
    xa, xb, x, gl, picks, tab, stab, sem,
):
    v = lax.axis_index("view")
    a_at = pl.multiple_of(jnp.clip(v - 2, 0, 5) * 8, 8)
    b_at = pl.multiple_of(jnp.clip(v - 1, 0, 5) * 8, 8)
    load_a = pltpu.make_async_copy(attrs.at[pl.ds(a_at, 8), :], xa, sem.at[0])
    load_b = pltpu.make_async_copy(attrs.at[pl.ds(b_at, 8), :], xb, sem.at[1])
    load_c = pltpu.make_async_copy(attrs.at[48:49, :], xb.at[0:1, :], sem.at[1])
    load_a.start()

    @pl.when(v < 7)
    def _():
        load_b.start()

    @pl.when(v == 7)
    def _():
        load_c.start()

    sub = lax.broadcasted_iota(jnp.int32, (8, 128), 0)
    lane = lax.broadcasted_iota(jnp.int32, (8, 128), 1)
    marks = mask[...].astype(jnp.float32).astype(jnp.bfloat16)
    i0 = lax.broadcasted_iota(jnp.int32, (128, 128), 0)
    i1 = lax.broadcasted_iota(jnp.int32, (128, 128), 1)
    upto = (i0 <= i1).astype(jnp.float32).astype(jnp.bfloat16)
    before = (i0 < i1).astype(jnp.float32).astype(jnp.bfloat16)
    after = (i0 > i1).astype(jnp.float32).astype(jnp.bfloat16)
    run = jnp.dot(marks, upto, preferred_element_type=jnp.float32).astype(jnp.int32)
    in_lanes = lax.dot_general(
        jnp.ones((8, 128), jnp.bfloat16), marks, (((1,), (1,)), ((), ())), preferred_element_type=jnp.float32
    )
    base = jnp.dot(in_lanes.astype(jnp.bfloat16), before, preferred_element_type=jnp.float32)
    end = base + in_lanes
    tab[...] = jnp.where(sub == 0, base, end).astype(jnp.int32)
    to_smem = pltpu.make_async_copy(tab, stab, sem.at[2])
    to_smem.start()
    total = jnp.sum(in_lanes, axis=1, keepdims=True)
    count[...] = jnp.broadcast_to(total, (8, 128)).astype(jnp.int32)

    in_row = jnp.dot(marks, jnp.ones((128, 128), jnp.bfloat16), preferred_element_type=jnp.float32)
    row_base = jnp.dot(after, in_row.astype(jnp.bfloat16), preferred_element_type=jnp.float32).astype(jnp.int32)
    e = jnp.where(mask[...] > 0, i1 + 128 + ((i1 - run + 1) << 8), 0)
    for bit in range(7):
        far = pltpu.roll(e, 128 - (1 << bit), axis=1)
        comes = (far & (256 << bit)) != 0
        goes = (e & (256 << bit)) != 0
        e = jnp.where(comes, far, jnp.where(goes, 0, e))
    e = e & 255
    turn = row_base & 127
    for bit in range(7):
        e = jnp.where((turn & (1 << bit)) != 0, pltpu.roll(e, 1 << bit, axis=1), e)
    picks[...] = e | jnp.where(i1 < turn, 256, 0)

    def step(c, _):
        s = pl.ds(pl.multiple_of(c * 1024, 1024), 1024)

        def row(ref, *at):
            return ref[at[:-1] + (slice(at[-1], at[-1] + 1), s)].reshape(8, 128)

        m = [row(means, i) for i in range(3)]
        sc = [row(scales, i) for i in range(3)]
        q = [row(quats, i) for i in range(4)]
        inv = 1.0 / jnp.sqrt(q[0] * q[0] + q[1] * q[1] + q[2] * q[2] + q[3] * q[3] + 0.25)
        w, xq, y, z = (t * inv for t in q)
        rq = [
            [1 - 2 * (y * y + z * z), 2 * (xq * y - w * z), 2 * (xq * z + w * y)],
            [2 * (xq * y + w * z), 1 - 2 * (xq * xq + z * z), 2 * (y * z - w * xq)],
            [2 * (xq * z - w * y), 2 * (y * z + w * xq), 1 - 2 * (xq * xq + y * y)],
        ]
        factor = [[rq[i][j] * sc[j] for j in range(3)] for i in range(3)]
        gbest = jnp.zeros((8, 128), jnp.float32)
        lbest = jnp.zeros((8, 128), jnp.float32)
        for n in range(seen.shape[0]):
            r = [[rot[i, n, j] for j in range(3)] for i in range(3)]
            p = [r[i][0] * m[0] + r[i][1] * m[1] + r[i][2] * m[2] + trans[n, i] for i in range(3)]
            near = 1.0 / jnp.maximum(p[2], 1.0)
            j00 = focal[n] * near
            j02 = -j00 * p[0] * near
            j12 = -j00 * p[1] * near
            first = [j00 * r[0][j] + j02 * r[2][j] for j in range(3)]
            second = [j00 * r[1][j] + j12 * r[2][j] for j in range(3)]
            pr = [sum(first[j] * factor[j][k] for j in range(3)) for k in range(3)]
            qr = [sum(second[j] * factor[j][k] for j in range(3)) for k in range(3)]
            a = pr[0] * pr[0] + pr[1] * pr[1] + pr[2] * pr[2] + 0.3
            cc = qr[0] * qr[0] + qr[1] * qr[1] + qr[2] * qr[2] + 0.3
            b = pr[0] * qr[0] + pr[1] * qr[1] + pr[2] * qr[2]
            half = 0.5 * (a - cc)
            lam = 0.5 * (a + cc) + jnp.sqrt(half * half + b * b + 0.01)
            on = row(seen, n) > 0
            g0, g1 = row(grad, n, 0), row(grad, n, 1)
            gbest = jnp.maximum(gbest, jnp.where(on, g0 * g0 + g1 * g1, 0.0))
            lbest = jnp.maximum(lbest, jnp.where(on, lam, 0.0))
        piece, at = c // 2, pl.multiple_of((c % 2) * 8, 8)
        part[piece, 0, pl.ds(at, 8), :] = gbest
        part[piece, 1, pl.ds(at, 8), :] = lbest
        gl[0:1, s] = gbest.reshape(1, 1024)
        gl[1:2, s] = lbest.reshape(1, 1024)
        return 0

    lax.fori_loop(0, 16, step, 0)

    load_a.wait()

    @pl.when(v < 7)
    def _():
        load_b.wait()

    @pl.when(v == 7)
    def _():
        load_c.wait()

    @pl.when(v == 0)
    def _():
        x[0:3, :] = means[...]
        x[3:6, :] = scales[...]
        x[6:8, :] = quats[0:2, :]

    @pl.when(v == 1)
    def _():
        x[0:2, :] = quats[2:4, :]
        x[2:8, :] = xb[0:6, :]

    @pl.when((v > 1) & (v < 7))
    def _():
        x[0:2, :] = xa[6:8, :]
        x[2:8, :] = xb[0:6, :]

    @pl.when(v == 7)
    def _():
        x[0:2, :] = xa[6:8, :]
        x[2:3, :] = xb[0:1, :]
        x[3:8, :] = jnp.zeros((5, G), jnp.float32)

    to_smem.wait()

    def pack(c, carry):
        block = stab[0, c] >> 7
        full = (stab[1, c] >> 7) > block
        cols = pl.ds(pl.multiple_of(c * 128, 128), 128)
        pick = jnp.broadcast_to(picks[pl.ds(c, 1), :], (8, 128))
        at, kind = pick & 127, pick & 384
        here, later = kind == 128, kind == 384
        done = []
        for ref, old in zip((x, gl), carry):
            got = jnp.take_along_axis(ref[:, cols], at, axis=1, mode="promise_in_bounds")
            now = jnp.where(here, got, old)
            done.append((now, jnp.where(full, jnp.where(later, got, 0.0), now)))
        tiles[block] = done[0][0]
        packed[block] = done[1][0][0:2]
        return done[0][1], done[1][1]

    zero = jnp.zeros((8, 128), jnp.float32)
    left = lax.fori_loop(0, 128, pack, (zero, zero), unroll=8)
    last = stab[1, 127]

    @pl.when(last < G)
    def _():
        tiles[last >> 7] = left[0]
        packed[last >> 7] = left[1][0:2]


def move_kernel(
    part, packed, tiles, count,
    out, best, counts,
    taken, takenp, merged, mergedp, allp, turned, tab, stab,
    s_part, r_part, s_pack, r_pack, s_best, r_best, s_all, r_all, s_count, r_count, s_pair, r_pair,
    s_own, r_own, s_side, r_side, s_far, r_far, own,
):
    v, g = lax.axis_index("view"), lax.axis_index("gauss")
    core, chip = v % 2, v // 2
    gy, gz = g // 8, g % 8
    barrier = pltpu.get_barrier_semaphore()
    each(1, NV, lambda i: pl.semaphore_signal(barrier, inc=1, device_id={"view": (v + i) % NV}, device_id_type=MESH))
    each(1, NG, lambda i: pl.semaphore_signal(barrier, inc=1, device_id={"gauss": (g + i) % NG}, device_id_type=MESH))
    pl.semaphore_wait(barrier, NV - 1 + NG - 1)

    def over_view(peer, src, dst, s, r):
        return pltpu.make_async_remote_copy(src, dst, s, r, device_id={"view": peer}, device_id_type=MESH)

    def over_gauss(peer, src, dst, s, r):
        return pltpu.make_async_remote_copy(src, dst, s, r, device_id={"gauss": peer}, device_id_type=MESH)

    def tell(i, slot):
        return over_gauss((g + i) % NG, count, counts.at[slot], s_count.at[i], r_count.at[slot])

    def give_part(i, slot):
        peer = (v + i) % NV
        return over_view(peer, part.at[peer], taken.at[slot], s_part.at[i], r_part.at[slot])

    def give_pack(i, slot):
        peer = (v + i) % NV
        src = packed.at[pl.ds(peer * 16, 16)]
        return over_view(peer, src, takenp.at[slot], s_pack.at[i], r_pack.at[slot])

    def give_best(i, slot):
        return over_view((v + i) % NV, merged, best.at[slot], s_best.at[i], r_best.at[slot])

    def give_all(slot):
        return over_view(NV - 1, mergedp, allp.at[pl.ds(slot * 16, 16)], s_all.at[0], r_all.at[slot])

    each(1, NG, lambda i: tell(i, g).start())
    each(1, NV, lambda i: give_pack(i, v).start())
    each(1, NV, lambda i: give_part(i, v).start())
    counts[g] = count[...]
    each(1, NG, lambda i: tell(i, (g + i) % NG).wait_recv())

    def add(s, mine):
        return mine + jnp.where(s < g, (counts[s] + (BLK - 1)) >> 7, 0)

    tab[...] = lax.fori_loop(0, NG, add, jnp.zeros((8, 128), jnp.int32))
    to_smem = pltpu.make_async_copy(tab, stab, own.at[0])
    to_smem.start()
    to_smem.wait()
    shift = stab[0, 0]

    rows = pl.ds(pl.multiple_of(v * 8, 8), 8)

    def span(at, size):
        return pl.ds(pl.multiple_of(at * size, size), size)

    def owner(i):
        return ((gy + i // 8) % 4) * 8 + (gz + i % 8) % 8

    def pair(i):
        return over_gauss(owner(i), turned.at[:, span(i, PAIR)], out.at[rows, span(i, PAIR)], s_pair.at[i], r_pair.at[i])

    keep = pltpu.make_async_copy(turned.at[:, 0:PAIR], out.at[rows, 0:PAIR], own.at[1])

    def turn(finish):
        def one(i, _):
            block = (owner(i) - shift) & (NG - 1)
            for w in range(PER):
                tile = finish(tiles[block + w * NG], block + w * NG)
                turned[:, span(i * PER + w, BLK)] = tile
            return 0

        lax.fori_loop(0, NG, one, 0)
        each(1, NG, lambda i: pair(i).start())
        keep.start()

    @pl.when(v < NV - 1)
    def _():
        turn(lambda tile, block: tile)

    each(1, NV, lambda i: give_pack(i, (v + i) % NV).wait_recv())

    def merge_p(i, top):
        return jnp.maximum(top, takenp[(v + i) % NV])

    topp = lax.fori_loop(1, NV, merge_p, packed[pl.ds(v * 16, 16)])
    mergedp[...] = topp

    @pl.when(v < NV - 1)
    def _():
        give_all(v).start()

    @pl.when(v == NV - 1)
    def _():
        allp[pl.ds(v * 16, 16)] = topp

    each(1, NV, lambda i: give_part(i, (v + i) % NV).wait_recv())

    def merge(i, top):
        return jnp.maximum(top, taken[(v + i) % NV])

    top = lax.fori_loop(1, NV, merge, part[v])
    merged[...] = top
    best[v] = top
    each(1, NV, lambda i: give_best(i, v).start())

    @pl.when(v == NV - 1)
    def _():
        each(0, NV - 1, lambda i: give_all(i).wait_recv())
        sub = lax.broadcasted_iota(jnp.int32, (8, 128), 0)

        def finish(tile, block):
            pair_rows = allp[block]
            gtop = jnp.broadcast_to(jnp.sqrt(pair_rows[0:1]), (8, 128))
            ltop = jnp.broadcast_to(3.0 * jnp.sqrt(pair_rows[1:2]), (8, 128))
            return jnp.where(sub == 3, gtop, jnp.where(sub == 4, ltop, tile))

        turn(finish)

    mate = chip * 2 + 1 - core
    right, left, far = (((chip + i) % 4) * 2 + core for i in (1, 3, 2))

    def cut(group, c):
        at = out.at[pl.ds(pl.multiple_of(group * 8, 8), 8), span(c, WIDE)]
        return at, at

    def side(kind, c, group):
        return over_view(mate, *cut(group, c), s_side.at[kind, c], r_side.at[kind, c])

    def go(way, c, group):
        peer = right if way == 0 else left
        return over_view(peer, *cut(group, c), s_own.at[way, c], r_own.at[way, c])

    def on(way, c, group):
        peer = right if way == 0 else left
        return over_view(peer, *cut(group, c), s_far.at[c], r_far.at[c])

    def a_step(c):
        @pl.when(c == 0)
        def _():
            keep.wait()

        each(jnp.where(c == 0, 1, c * 4), c * 4 + 4, lambda i: pair(i).wait_recv())
        go(0, c, v).start()
        go(1, c, v).start()
        side(0, c, v).start()

    def b_step(c):
        go(0, c, left).wait_recv()

        @pl.when(c < CHUNKS // 2)
        def _():
            on(0, c, left).start()

        side(2, c, left).start()
        go(1, c, right).wait_recv()

        @pl.when(c >= CHUNKS // 2)
        def _():
            on(1, c, right).start()

        side(1, c, right).start()

    def c_step(c):
        on(0, c, far).wait_recv()
        side(3, c, far).start()

    lag_b, lag_c = 3, 5

    def stage(t):
        @pl.when(t < CHUNKS)
        def _():
            a_step(t)

        @pl.when((t >= lag_b) & (t < CHUNKS + lag_b))
        def _():
            b_step(t - lag_b)

        @pl.when(t >= lag_c)
        def _():
            c_step(t - lag_c)

    each(0, CHUNKS + lag_c, stage)

    across = [mate, right + 1 - 2 * core, left + 1 - 2 * core, far + 1 - 2 * core]
    for kind in range(4):
        each(0, CHUNKS, lambda c: side(kind, c, across[kind]).wait_recv())
    each(1, NV, lambda i: give_best(i, (v + i) % NV).wait_recv())

    each(1, NG, lambda i: tell(i, g).wait_send())
    each(1, NG, lambda i: pair(i).wait_send())
    each(1, NV, lambda i: give_part(i, v).wait_send())
    each(1, NV, lambda i: give_pack(i, v).wait_send())
    each(1, NV, lambda i: give_best(i, v).wait_send())

    @pl.when(v < NV - 1)
    def _():
        give_all(v).wait_send()

    for kind in range(4):
        each(0, CHUNKS, lambda c: side(kind, c, v).wait_send())
    each(0, CHUNKS, lambda c: go(0, c, v).wait_send())
    each(0, CHUNKS, lambda c: go(1, c, v).wait_send())
    each(0, CHUNKS, lambda c: on(0, c, v).wait_send())


def lay_kernel(counts, best, tiles, clones, peak, total, stage, tab, stab, sem):
    g = lax.axis_index("gauss")
    gy, gz = g // 8, g % 8
    sub = lax.broadcasted_iota(jnp.int32, (8, 128), 0)
    k = lax.broadcasted_iota(jnp.int32, (8, 128), 1) * NG + g
    off = jnp.zeros((8, 128), jnp.int32)
    every = jnp.zeros((8, 128), jnp.int32)
    source = jnp.zeros((8, 128), jnp.int32)
    for s in range(NG):
        n = counts[s]
        blocks = (n + (BLK - 1)) >> 7
        where = (((gy - s // 8) & 3) * 8 + ((gz - s % 8) & 7)) * PER
        inside = (k >= off) & (k < off + blocks)
        source = jnp.where(inside, where + ((k - off) >> 5), source)
        off = off + blocks
        every = every + n
    slots = (off - g + (NG - 1)) >> 5
    tab[...] = jnp.where(sub == 0, source, jnp.where(sub == 1, every, slots))
    to_smem = pltpu.make_async_copy(tab, stab, sem.at[0])
    to_smem.start()
    to_smem.wait()
    used = stab[2, 0]
    total[0, 0] = stab[1, 0]

    def cols(at):
        return pl.ds(pl.multiple_of(at * BLK, BLK), BLK)

    def fetch(q):
        return pltpu.make_async_copy(tiles.at[:, cols(stab[0, q])], stage.at[:, cols(q)], sem.at[1])

    each(0, used, lambda q: fetch(q).start())

    def clear(q):
        stage[:, cols(q)] = jnp.zeros((8 * NV, BLK), jnp.float32)

    each(used, CAP, clear)

    def roots(c, _):
        s = pl.ds(pl.multiple_of(c * 1024, 1024), 1024)
        piece, at = c // 2, pl.multiple_of((c % 2) * 8, 8)
        peak[0:1, s] = jnp.sqrt(best[piece, 0, pl.ds(at, 8), :]).reshape(1, 1024)
        peak[1:2, s] = (3.0 * jnp.sqrt(best[piece, 1, pl.ds(at, 8), :])).reshape(1, 1024)
        return 0

    lax.fori_loop(0, 16, roots, 0)
    each(0, used, lambda q: fetch(q).wait())

    puts = []
    for r in range(NV):
        lo, hi = 8 * r, min(8 * r + 8, ROWS)
        puts.append(pltpu.make_async_copy(stage.at[lo:hi, :], clones.at[lo:hi, :], sem.at[2 + r]))
    for put in puts:
        put.start()
    for put in puts:
        put.wait()


def body(means, scales, quats, attrs, grad_screen, visible, clone_mask, rotation, shift, focal):
    f32, i32 = jnp.float32, jnp.int32
    shape = jax.ShapeDtypeStruct
    dma = pltpu.SemaphoreType.DMA
    mask = clone_mask.reshape(128, 128)
    part, packed, tiles, count = pl.pallas_call(
        front_kernel,
        in_specs=[VMEM] * 6 + [SMEM] * 3 + [ANY],
        out_specs=(VMEM,) * 4,
        out_shape=(
            shape((NV, 2, 16, 128), f32),
            shape((CAP, 2, 128), f32),
            shape((CAP, 8, 128), f32),
            shape((8, 128), i32),
        ),
        scratch_shapes=[
            pltpu.VMEM((8, G), f32),
            pltpu.VMEM((8, G), f32),
            pltpu.VMEM((8, G), f32),
            pltpu.VMEM((8, G), f32),
            pltpu.VMEM((128, 128), i32),
            pltpu.VMEM((8, 128), i32),
            pltpu.SMEM((8, 128), i32),
            dma((3,)),
        ],
        compiler_params=pltpu.CompilerParams(vmem_limit_bytes=16 * 2**20),
        name="front",
    )(mask, means, scales, quats, grad_screen, visible, rotation.transpose(1, 0, 2), shift, focal, attrs)

    out, best, counts = pl.pallas_call(
        move_kernel,
        in_specs=[VMEM] * 4,
        out_specs=(ANY, VMEM, VMEM),
        out_shape=(
            shape((8 * NV, G), f32),
            shape((NV, 2, 16, 128), f32),
            shape((NG, 8, 128), i32),
        ),
        scratch_shapes=[
            pltpu.VMEM((NV, 2, 16, 128), f32),
            pltpu.VMEM((NV, 16, 2, 128), f32),
            pltpu.VMEM((2, 16, 128), f32),
            pltpu.VMEM((16, 2, 128), f32),
            pltpu.VMEM((CAP, 2, 128), f32),
            pltpu.VMEM((8, G), f32),
            pltpu.VMEM((8, 128), i32),
            pltpu.SMEM((8, 128), i32),
        ]
        + [dma((NV,))] * 6
        + [dma((1,)), dma((NV,))]
        + [dma((NG,))] * 4
        + [dma((2, CHUNKS)), dma((2, CHUNKS)), dma((4, CHUNKS)), dma((4, CHUNKS)), dma((CHUNKS,)), dma((CHUNKS,))]
        + [dma((2,))],
        compiler_params=pltpu.CompilerParams(
            collective_id=0, has_side_effects=True, vmem_limit_bytes=16 * 2**20
        ),
        name="move",
    )(part, packed, tiles, count)

    clones, peak, total = pl.pallas_call(
        lay_kernel,
        in_specs=[VMEM, VMEM, ANY],
        out_specs=(ANY, VMEM, SMEM),
        out_shape=(shape((ROWS, G), f32), shape((2, G), f32), shape((1, 1), i32)),
        scratch_shapes=[
            pltpu.VMEM((8 * NV, G), f32),
            pltpu.VMEM((8, 128), i32),
            pltpu.SMEM((8, 128), i32),
            dma((2 + NV,)),
        ],
        compiler_params=pltpu.CompilerParams(vmem_limit_bytes=16 * 2**20),
        name="lay",
    )(counts, best, out)
    return (peak, clones, total.reshape(()))


def solution(mesh):
    return jax.shard_map(
        body,
        mesh=mesh,
        in_specs=(
            P(None, "gauss"),
            P(None, "gauss"),
            P(None, "gauss"),
            P(None, "gauss"),
            P("view", None, "gauss"),
            P("view", "gauss"),
            P("gauss"),
            P("view", None, None),
            P("view", None),
            P("view"),
        ),
        out_specs=(P(None, "gauss"), P(None, "gauss"), P()),
        check_vma=False,
    )
```

```python
import jax
import jax.numpy as jnp
from jax import lax
from jax.experimental import pallas as pl
from jax.experimental.pallas import tpu as pltpu
from jax.sharding import PartitionSpec as P

G = 16384
ROWS = 61
BLK = 128
CAP = G // BLK
NV = 8
NG = 32
PER = CAP // NG
PAIR = PER * BLK
CHUNKS = 8
WIDE = G // CHUNKS
LAG_B, LAG_C = 3, 5
MESH = pl.DeviceIdType.MESH
VMEM = pl.BlockSpec(memory_space=pltpu.VMEM)
SMEM = pl.BlockSpec(memory_space=pltpu.SMEM)
ANY = pl.BlockSpec(memory_space=pl.ANY)
HBM = pl.BlockSpec(memory_space=pltpu.HBM)


def each(lo, n, do):
    def one(i, _):
        do(i)
        return 0

    lax.fori_loop(lo, n, one, 0)


def front_kernel(
    mask_h, means_h, scales_h, quats_h, grad_h, seen_h, rot_h, trans_h, focal_h, attrs,
    part, packed, tiles, count, blank,
    mask, means, scales, quats, grad, seen, rot, trans, focal,
    xa, xb, x, gl, picks, tab, stab, zeros, sem, load_sem, blank_sem,
):
    v = lax.axis_index("view")
    pairs = (
        (mask_h, mask), (rot_h, rot), (trans_h, trans), (focal_h, focal), (means_h, means), (scales_h, scales),
        (quats_h, quats), (seen_h, seen), (grad_h, grad),
    )
    loads = [pltpu.make_async_copy(src, dst, load_sem.at[i]) for i, (src, dst) in enumerate(pairs)]
    for load in loads:
        load.start()
    a_at = pl.multiple_of(jnp.clip(v - 2, 0, 5) * 8, 8)
    b_at = pl.multiple_of(jnp.clip(v - 1, 0, 5) * 8, 8)
    load_a = pltpu.make_async_copy(attrs.at[pl.ds(a_at, 8), :], xa, sem.at[0])
    load_b = pltpu.make_async_copy(attrs.at[pl.ds(b_at, 8), :], xb, sem.at[1])
    load_c = pltpu.make_async_copy(attrs.at[48:49, :], xb.at[0:1, :], sem.at[1])
    load_a.start()

    @pl.when(v < 7)
    def _():
        load_b.start()

    @pl.when(v == 7)
    def _():
        load_c.start()

    zeros[...] = jnp.zeros_like(zeros)
    fills = []
    for r in range(NV):
        lo, hi = 8 * r, min(8 * r + 8, ROWS)
        fills.append(pltpu.make_async_copy(zeros.at[0 : hi - lo, :], blank.at[lo:hi, :], blank_sem.at[r]))
    loads[0].wait()

    sub = lax.broadcasted_iota(jnp.int32, (8, 128), 0)
    lane = lax.broadcasted_iota(jnp.int32, (8, 128), 1)
    marks = mask[...].astype(jnp.float32).astype(jnp.bfloat16)
    i0 = lax.broadcasted_iota(jnp.int32, (128, 128), 0)
    i1 = lax.broadcasted_iota(jnp.int32, (128, 128), 1)
    upto = (i0 <= i1).astype(jnp.float32).astype(jnp.bfloat16)
    before = (i0 < i1).astype(jnp.float32).astype(jnp.bfloat16)
    after = (i0 > i1).astype(jnp.float32).astype(jnp.bfloat16)
    run = jnp.dot(marks, upto, preferred_element_type=jnp.float32).astype(jnp.int32)
    in_lanes = lax.dot_general(
        jnp.ones((8, 128), jnp.bfloat16), marks, (((1,), (1,)), ((), ())), preferred_element_type=jnp.float32
    )
    base = jnp.dot(in_lanes.astype(jnp.bfloat16), before, preferred_element_type=jnp.float32)
    end = base + in_lanes
    tab[...] = jnp.where(sub == 0, base, end).astype(jnp.int32)
    to_smem = pltpu.make_async_copy(tab, stab, sem.at[2])
    to_smem.start()
    total = jnp.sum(in_lanes, axis=1, keepdims=True)
    count[...] = jnp.broadcast_to(total, (8, 128)).astype(jnp.int32)

    in_row = jnp.dot(marks, jnp.ones((128, 128), jnp.bfloat16), preferred_element_type=jnp.float32)
    row_base = jnp.dot(after, in_row.astype(jnp.bfloat16), preferred_element_type=jnp.float32).astype(jnp.int32)
    e = jnp.where(mask[...] > 0, i1 + 128 + ((i1 - run + 1) << 8), 0)
    for bit in range(7):
        far = pltpu.roll(e, 128 - (1 << bit), axis=1)
        comes = (far & (256 << bit)) != 0
        goes = (e & (256 << bit)) != 0
        e = jnp.where(comes, far, jnp.where(goes, 0, e))
    e = e & 255
    turn = row_base & 127
    for bit in range(7):
        e = jnp.where((turn & (1 << bit)) != 0, pltpu.roll(e, 1 << bit, axis=1), e)
    picks[...] = e | jnp.where(i1 < turn, 256, 0)

    for load in loads[1:]:
        load.wait()
    for fill in fills:
        fill.start()

    def step(c, _):
        s = pl.ds(pl.multiple_of(c * 1024, 1024), 1024)

        def row(ref, *at):
            return ref[at[:-1] + (slice(at[-1], at[-1] + 1), s)].reshape(8, 128)

        m = [row(means, i) for i in range(3)]
        sc = [row(scales, i) for i in range(3)]
        q = [row(quats, i) for i in range(4)]
        inv = 1.0 / jnp.sqrt(q[0] * q[0] + q[1] * q[1] + q[2] * q[2] + q[3] * q[3] + 0.25)
        w, xq, y, z = (t * inv for t in q)
        rq = [
            [1 - 2 * (y * y + z * z), 2 * (xq * y - w * z), 2 * (xq * z + w * y)],
            [2 * (xq * y + w * z), 1 - 2 * (xq * xq + z * z), 2 * (y * z - w * xq)],
            [2 * (xq * z - w * y), 2 * (y * z + w * xq), 1 - 2 * (xq * xq + y * y)],
        ]
        factor = [[rq[i][j] * sc[j] for j in range(3)] for i in range(3)]
        gbest = jnp.zeros((8, 128), jnp.float32)
        lbest = jnp.zeros((8, 128), jnp.float32)
        for n in range(seen.shape[0]):
            r = [[rot[i, n, j] for j in range(3)] for i in range(3)]
            p = [r[i][0] * m[0] + r[i][1] * m[1] + r[i][2] * m[2] + trans[n, i] for i in range(3)]
            near = 1.0 / jnp.maximum(p[2], 1.0)
            j00 = focal[n] * near
            j02 = -j00 * p[0] * near
            j12 = -j00 * p[1] * near
            first = [j00 * r[0][j] + j02 * r[2][j] for j in range(3)]
            second = [j00 * r[1][j] + j12 * r[2][j] for j in range(3)]
            pr = [sum(first[j] * factor[j][k] for j in range(3)) for k in range(3)]
            qr = [sum(second[j] * factor[j][k] for j in range(3)) for k in range(3)]
            a = pr[0] * pr[0] + pr[1] * pr[1] + pr[2] * pr[2] + 0.3
            cc = qr[0] * qr[0] + qr[1] * qr[1] + qr[2] * qr[2] + 0.3
            b = pr[0] * qr[0] + pr[1] * qr[1] + pr[2] * qr[2]
            half = 0.5 * (a - cc)
            lam = 0.5 * (a + cc) + jnp.sqrt(half * half + b * b + 0.01)
            on = row(seen, n) > 0
            g0, g1 = row(grad, n, 0), row(grad, n, 1)
            gbest = jnp.maximum(gbest, jnp.where(on, g0 * g0 + g1 * g1, 0.0))
            lbest = jnp.maximum(lbest, jnp.where(on, lam, 0.0))
        piece, at = c // 2, pl.multiple_of((c % 2) * 8, 8)
        part[piece, 0, pl.ds(at, 8), :] = gbest
        part[piece, 1, pl.ds(at, 8), :] = lbest
        gl[0:1, s] = gbest.reshape(1, 1024)
        gl[1:2, s] = lbest.reshape(1, 1024)
        return 0

    lax.fori_loop(0, 16, step, 0)

    load_a.wait()

    @pl.when(v < 7)
    def _():
        load_b.wait()

    @pl.when(v == 7)
    def _():
        load_c.wait()

    @pl.when(v == 0)
    def _():
        x[0:3, :] = means[...]
        x[3:6, :] = scales[...]
        x[6:8, :] = quats[0:2, :]

    @pl.when(v == 1)
    def _():
        x[0:2, :] = quats[2:4, :]
        x[2:8, :] = xb[0:6, :]

    @pl.when((v > 1) & (v < 7))
    def _():
        x[0:2, :] = xa[6:8, :]
        x[2:8, :] = xb[0:6, :]

    @pl.when(v == 7)
    def _():
        x[0:2, :] = xa[6:8, :]
        x[2:3, :] = xb[0:1, :]
        x[3:8, :] = jnp.zeros((5, G), jnp.float32)

    to_smem.wait()

    def pack(c, carry):
        block = stab[0, c] >> 7
        full = (stab[1, c] >> 7) > block
        cols = pl.ds(pl.multiple_of(c * 128, 128), 128)
        pick = jnp.broadcast_to(picks[pl.ds(c, 1), :], (8, 128))
        at, kind = pick & 127, pick & 384
        here, later = kind == 128, kind == 384
        done = []
        for ref, old in zip((x, gl), carry):
            got = jnp.take_along_axis(ref[:, cols], at, axis=1, mode="promise_in_bounds")
            now = jnp.where(here, got, old)
            done.append((now, jnp.where(full, jnp.where(later, got, 0.0), now)))
        tiles[block] = done[0][0]
        packed[block] = done[1][0][0:2]
        return done[0][1], done[1][1]

    zero = jnp.zeros((8, 128), jnp.float32)
    left = lax.fori_loop(0, 128, pack, (zero, zero), unroll=8)
    last = stab[1, 127]

    @pl.when(last < G)
    def _():
        tiles[last >> 7] = left[0]
        packed[last >> 7] = left[1][0:2]

    for fill in fills:
        fill.wait()


def move_kernel(
    part, packed, tiles, count,
    out, peaks, best, counts,
    taken, takenp, merged, mergedp, ownp, turned, turnedp, tab, stab,
    s_part, r_part, s_pack, r_pack, s_best, r_best, s_peak, r_peak, s_count, r_count, s_pair, r_pair, s_top, r_top,
    s_own, r_own, s_side, r_side, s_far, r_far, own,
):
    v, g = lax.axis_index("view"), lax.axis_index("gauss")
    core, chip = v % 2, v // 2
    gy, gz = g // 8, g % 8
    barrier = pltpu.get_barrier_semaphore()
    each(1, NV, lambda i: pl.semaphore_signal(barrier, inc=1, device_id={"view": (v + i) % NV}, device_id_type=MESH))
    each(1, NG, lambda i: pl.semaphore_signal(barrier, inc=1, device_id={"gauss": (g + i) % NG}, device_id_type=MESH))
    pl.semaphore_wait(barrier, NV - 1 + NG - 1)

    def over_view(peer, src, dst, s, r):
        return pltpu.make_async_remote_copy(src, dst, s, r, device_id={"view": peer}, device_id_type=MESH)

    def over_gauss(peer, src, dst, s, r):
        return pltpu.make_async_remote_copy(src, dst, s, r, device_id={"gauss": peer}, device_id_type=MESH)

    def span(at, size):
        return pl.ds(pl.multiple_of(at * size, size), size)

    def owner(i):
        return ((gy + i // 8) % 4) * 8 + (gz + i % 8) % 8

    def tell(i, slot):
        return over_gauss((g + i) % NG, count, counts.at[slot], s_count.at[i], r_count.at[slot])

    def give_part(i, slot):
        peer = (v + i) % NV
        return over_view(peer, part.at[peer], taken.at[slot], s_part.at[i], r_part.at[slot])

    def give_best(i, slot):
        return over_view((v + i) % NV, merged, best.at[slot], s_best.at[i], r_best.at[slot])

    def give_pack(i, slot):
        peer = (v + i) % NV
        return over_view(peer, turnedp.at[pl.ds(peer * 16, 16)], takenp.at[slot], s_pack.at[i], r_pack.at[slot])

    def give_top(t):
        at = pl.ds(t * PER, PER)
        return over_gauss(owner(v * 4 + t), mergedp.at[at], ownp.at[at], s_top.at[t], r_top.at[t])

    def give_peak(i, slot):
        return over_view((v + i) % NV, ownp, peaks.at[pl.ds(slot * 16, 16)], s_peak.at[i], r_peak.at[slot])

    each(1, NG, lambda i: tell(i, g).start())
    each(1, NV, lambda i: give_part(i, v).start())
    counts[g] = count[...]
    each(1, NG, lambda i: tell(i, (g + i) % NG).wait_recv())

    def add(s, mine):
        return mine + jnp.where(s < g, (counts[s] + (BLK - 1)) >> 7, 0)

    tab[...] = lax.fori_loop(0, NG, add, jnp.zeros((8, 128), jnp.int32))
    to_smem = pltpu.make_async_copy(tab, stab, own.at[0])
    to_smem.start()
    to_smem.wait()
    shift = stab[0, 0]

    rows = pl.ds(pl.multiple_of(v * 8, 8), 8)

    def pair(i):
        return over_gauss(owner(i), turned.at[:, span(i, PAIR)], out.at[rows, span(i, PAIR)], s_pair.at[i], r_pair.at[i])

    keep = pltpu.make_async_copy(turned.at[:, 0:PAIR], out.at[rows, 0:PAIR], own.at[1])

    def turn(i):
        block = (owner(i) - shift) & (NG - 1)
        for w in range(PER):
            turned[:, span(i * PER + w, BLK)] = tiles[block + w * NG]
            turnedp[i * PER + w] = packed[block + w * NG]

    each(0, NG, turn)
    each(1, NG, lambda i: pair(i).start())
    keep.start()
    each(1, NV, lambda i: give_pack(i, v).start())

    mate = chip * 2 + 1 - core
    right, left, far = (((chip + i) % 4) * 2 + core for i in (1, 3, 2))

    def cut(group, c):
        at = out.at[pl.ds(pl.multiple_of(group * 8, 8), 8), span(c, WIDE)]
        return at, at

    def side(kind, c, group):
        return over_view(mate, *cut(group, c), s_side.at[kind, c], r_side.at[kind, c])

    def go(way, c, group):
        peer = right if way == 0 else left
        return over_view(peer, *cut(group, c), s_own.at[way, c], r_own.at[way, c])

    def on(way, c, group):
        peer = right if way == 0 else left
        return over_view(peer, *cut(group, c), s_far.at[c], r_far.at[c])

    def a_step(c):
        if c == 0:
            keep.wait()
        each(max(c * 4, 1), c * 4 + 4, lambda i: pair(i).wait_recv())
        go(0, c, v).start()
        go(1, c, v).start()
        side(0, c, v).start()

    def b_step(c):
        go(0, c, left).wait_recv()
        if c < CHUNKS // 2:
            on(0, c, left).start()
        side(2, c, left).start()
        go(1, c, right).wait_recv()
        if c >= CHUNKS // 2:
            on(1, c, right).start()
        side(1, c, right).start()

    def c_step(c):
        on(0, c, far).wait_recv()
        side(3, c, far).start()

    def first():
        each(1, NV, lambda i: give_part(i, (v + i) % NV).wait_recv())
        top = lax.fori_loop(1, NV, lambda i, top: jnp.maximum(top, taken[(v + i) % NV]), part[v])
        merged[...] = top
        best[v] = top
        each(1, NV, lambda i: give_best(i, v).start())

    def second():
        each(1, NV, lambda i: give_pack(i, (v + i) % NV).wait_recv())
        top = lax.fori_loop(1, NV, lambda i, top: jnp.maximum(top, takenp[(v + i) % NV]), turnedp[pl.ds(v * 16, 16)])
        mergedp[...] = top

        @pl.when(v > 0)
        def _():
            give_top(0).start()

        @pl.when(v == 0)
        def _():
            ownp[0:PER] = top[0:PER]

        each(1, 4, lambda t: give_top(t).start())

    def third():
        @pl.when(v > 0)
        def _():
            give_top(0).wait_recv()

        each(1, 4, lambda t: give_top(t).wait_recv())
        peaks[pl.ds(v * 16, 16)] = ownp[...]
        each(1, NV, lambda i: give_peak(i, v).start())

    between = {0: first, 2: second, 5: third}
    for t in range(CHUNKS + LAG_C):
        if t < CHUNKS:
            a_step(t)
        if LAG_B <= t < CHUNKS + LAG_B:
            b_step(t - LAG_B)
        if LAG_C <= t:
            c_step(t - LAG_C)
        if t in between:
            between[t]()

    across = [mate, right + 1 - 2 * core, left + 1 - 2 * core, far + 1 - 2 * core]
    for kind in range(4):
        each(0, CHUNKS, lambda c: side(kind, c, across[kind]).wait_recv())
    each(1, NV, lambda i: give_best(i, (v + i) % NV).wait_recv())
    each(1, NV, lambda i: give_peak(i, (v + i) % NV).wait_recv())

    each(1, NG, lambda i: tell(i, g).wait_send())
    each(1, NG, lambda i: pair(i).wait_send())
    each(1, NV, lambda i: give_part(i, v).wait_send())
    each(1, NV, lambda i: give_pack(i, v).wait_send())
    each(1, NV, lambda i: give_best(i, v).wait_send())
    each(1, NV, lambda i: give_peak(i, v).wait_send())

    @pl.when(v > 0)
    def _():
        give_top(0).wait_send()

    each(1, 4, lambda t: give_top(t).wait_send())
    for kind in range(4):
        each(0, CHUNKS, lambda c: side(kind, c, v).wait_send())
    each(0, CHUNKS, lambda c: go(0, c, v).wait_send())
    each(0, CHUNKS, lambda c: go(1, c, v).wait_send())
    each(0, CHUNKS, lambda c: on(0, c, v).wait_send())


def lay_kernel(counts, best, peaks, tiles, blank, clones, peak, total, stage, tab, stab, sem):
    del blank
    g = lax.axis_index("gauss")
    gy, gz = g // 8, g % 8
    sub = lax.broadcasted_iota(jnp.int32, (8, 128), 0)
    k = lax.broadcasted_iota(jnp.int32, (8, 128), 1) * NG + g
    off = jnp.zeros((8, 128), jnp.int32)
    every = jnp.zeros((8, 128), jnp.int32)
    source = jnp.zeros((8, 128), jnp.int32)
    for s in range(NG):
        n = counts[s]
        blocks = (n + (BLK - 1)) >> 7
        where = (((gy - s // 8) & 3) * 8 + ((gz - s % 8) & 7)) * PER
        inside = (k >= off) & (k < off + blocks)
        source = jnp.where(inside, where + ((k - off) >> 5), source)
        off = off + blocks
        every = every + n
    slots = (off - g + (NG - 1)) >> 5
    tab[...] = jnp.where(sub == 0, source, jnp.where(sub == 1, every, slots))
    to_smem = pltpu.make_async_copy(tab, stab, sem.at[0])
    to_smem.start()
    to_smem.wait()
    used = stab[2, 0]
    total[0, 0] = stab[1, 0]

    def cols(at):
        return pl.ds(pl.multiple_of(at * BLK, BLK), BLK)

    def put(q):
        return pltpu.make_async_copy(tiles.at[0:56, cols(stab[0, q])], clones.at[0:56, cols(q)], sem.at[1])

    def put_last(q):
        return pltpu.make_async_copy(stage.at[0 : ROWS - 56, cols(q)], clones.at[56:ROWS, cols(q)], sem.at[2])

    each(0, used, lambda q: put(q).start())

    def finish(q):
        at = stab[0, q]
        tops = peaks[at]
        gtop = jnp.broadcast_to(jnp.sqrt(tops[0:1]), (8, 128))
        ltop = jnp.broadcast_to(3.0 * jnp.sqrt(tops[1:2]), (8, 128))
        tile = tiles[56:64, cols(at)]
        stage[:, cols(q)] = jnp.where(sub == 3, gtop, jnp.where(sub == 4, ltop, tile))

    each(0, used, finish)
    each(0, used, lambda q: put_last(q).start())

    def roots(c, _):
        s = pl.ds(pl.multiple_of(c * 1024, 1024), 1024)
        piece, at = c // 2, pl.multiple_of((c % 2) * 8, 8)
        peak[0:1, s] = jnp.sqrt(best[piece, 0, pl.ds(at, 8), :]).reshape(1, 1024)
        peak[1:2, s] = (3.0 * jnp.sqrt(best[piece, 1, pl.ds(at, 8), :])).reshape(1, 1024)
        return 0

    lax.fori_loop(0, 16, roots, 0)
    each(0, used, lambda q: put(q).wait())
    each(0, used, lambda q: put_last(q).wait())


def body(means, scales, quats, attrs, grad_screen, visible, clone_mask, rotation, shift, focal):
    f32, i32 = jnp.float32, jnp.int32
    shape = jax.ShapeDtypeStruct
    dma = pltpu.SemaphoreType.DMA
    mask = clone_mask.reshape(128, 128)
    part, packed, tiles, count, blank = pl.pallas_call(
        front_kernel,
        in_specs=[HBM] * 10,
        out_specs=(VMEM,) * 4 + (HBM,),
        out_shape=(
            shape((NV, 2, 16, 128), f32),
            shape((CAP, 2, 128), f32),
            shape((CAP, 8, 128), f32),
            shape((8, 128), i32),
            shape((ROWS, G), f32),
        ),
        scratch_shapes=[
            pltpu.VMEM((128, 128), i32),
            pltpu.VMEM((3, G), f32),
            pltpu.VMEM((3, G), f32),
            pltpu.VMEM((4, G), f32),
            pltpu.VMEM((4, 2, G), f32),
            pltpu.VMEM((4, G), i32),
            pltpu.SMEM((3, 4, 3), f32),
            pltpu.SMEM((4, 3), f32),
            pltpu.SMEM((4,), f32),
            pltpu.VMEM((8, G), f32),
            pltpu.VMEM((8, G), f32),
            pltpu.VMEM((8, G), f32),
            pltpu.VMEM((8, G), f32),
            pltpu.VMEM((128, 128), i32),
            pltpu.VMEM((8, 128), i32),
            pltpu.SMEM((8, 128), i32),
            pltpu.VMEM((8, G), f32),
            dma((3,)),
            dma((9,)),
            dma((NV,)),
        ],
        compiler_params=pltpu.CompilerParams(vmem_limit_bytes=16 * 2**20),
        name="front",
    )(
        *(
            pltpu.with_memory_space_constraint(a, pltpu.HBM)
            for a in (mask, means, scales, quats, grad_screen, visible, rotation.transpose(1, 0, 2), shift, focal, attrs)
        )
    )

    out, peaks, best, counts = pl.pallas_call(
        move_kernel,
        in_specs=[VMEM] * 4,
        out_specs=(VMEM, VMEM, VMEM, VMEM),
        out_shape=(
            shape((8 * NV, G), f32),
            shape((CAP, 2, 128), f32),
            shape((NV, 2, 16, 128), f32),
            shape((NG, 8, 128), i32),
        ),
        scratch_shapes=[
            pltpu.VMEM((NV, 2, 16, 128), f32),
            pltpu.VMEM((NV, 16, 2, 128), f32),
            pltpu.VMEM((2, 16, 128), f32),
            pltpu.VMEM((16, 2, 128), f32),
            pltpu.VMEM((16, 2, 128), f32),
            pltpu.VMEM((8, G), f32),
            pltpu.VMEM((CAP, 2, 128), f32),
            pltpu.VMEM((8, 128), i32),
            pltpu.SMEM((8, 128), i32),
        ]
        + [dma((NV,))] * 8
        + [dma((NG,))] * 4
        + [dma((4,))] * 2
        + [dma((2, CHUNKS)), dma((2, CHUNKS)), dma((4, CHUNKS)), dma((4, CHUNKS)), dma((CHUNKS,)), dma((CHUNKS,))]
        + [dma((2,))],
        compiler_params=pltpu.CompilerParams(
            collective_id=0, has_side_effects=True, vmem_limit_bytes=16 * 2**20
        ),
        name="move",
    )(part, packed, tiles, count)

    clones, peak, total = pl.pallas_call(
        lay_kernel,
        in_specs=[VMEM, VMEM, VMEM, VMEM, HBM],
        out_specs=(HBM, VMEM, SMEM),
        out_shape=(shape((ROWS, G), f32), shape((2, G), f32), shape((1, 1), i32)),
        input_output_aliases={4: 0},
        scratch_shapes=[
            pltpu.VMEM((8, G), f32),
            pltpu.VMEM((8, 128), i32),
            pltpu.SMEM((8, 128), i32),
            dma((3,)),
        ],
        compiler_params=pltpu.CompilerParams(vmem_limit_bytes=16 * 2**20),
        name="lay",
    )(counts, best, peaks, out, blank)
    return (peak, clones, total.reshape(()))


def solution(mesh):
    return jax.shard_map(
        body,
        mesh=mesh,
        in_specs=(
            P(None, "gauss"),
            P(None, "gauss"),
            P(None, "gauss"),
            P(None, "gauss"),
            P("view", None, "gauss"),
            P("view", "gauss"),
            P("gauss"),
            P("view", None, None),
            P("view", None),
            P("view"),
        ),
        out_specs=(P(None, "gauss"), P(None, "gauss"), P()),
        check_vma=False,
    )
```

```python
import functools

import jax
import jax.numpy as jnp
from jax import lax
from jax.experimental import pallas as pl
from jax.experimental.pallas import tpu as pltpu
from jax.sharding import PartitionSpec as P

G = 16384
ROWS = 61
BLK = 128
CAP = G // BLK
NV = 8
NG = 32
PER = CAP // NG
CHUNKS = 4
SIZES = (32, 40, 48, 56, 64, 96, 128)
MESH = pl.DeviceIdType.MESH
VMEM = pl.BlockSpec(memory_space=pltpu.VMEM)
SMEM = pl.BlockSpec(memory_space=pltpu.SMEM)
HBM = pl.BlockSpec(memory_space=pltpu.HBM)


def each(lo, n, do):
    if isinstance(lo, int) and isinstance(n, int):
        for i in range(lo, n):
            do(i)
        return

    def one(i, _):
        do(i)
        return 0

    lax.fori_loop(lo, n, one, 0)


def front_kernel(
    mask_h, means_h, scales_h, quats_h, grad_h, seen_h, rot_h, trans_h, focal_h, attrs,
    part, packed, tiles, count, blank,
    mask, means, scales, quats, grad, seen, rot, trans, focal,
    xa, xb, x, gl, picks, tab, stab, zeros, sem, load_sem, blank_sem,
):
    v = lax.axis_index("view")
    pairs = (
        (mask_h, mask), (rot_h, rot), (trans_h, trans), (focal_h, focal), (means_h, means), (scales_h, scales),
        (quats_h, quats), (seen_h, seen), (grad_h, grad),
    )
    loads = [pltpu.make_async_copy(src, dst, load_sem.at[i]) for i, (src, dst) in enumerate(pairs)]
    for load in loads:
        load.start()
    a_at = pl.multiple_of(jnp.clip(v - 2, 0, 5) * 8, 8)
    b_at = pl.multiple_of(jnp.clip(v - 1, 0, 5) * 8, 8)
    load_a = pltpu.make_async_copy(attrs.at[pl.ds(a_at, 8), :], xa, sem.at[0])
    load_b = pltpu.make_async_copy(attrs.at[pl.ds(b_at, 8), :], xb, sem.at[1])
    load_c = pltpu.make_async_copy(attrs.at[48:49, :], xb.at[0:1, :], sem.at[1])
    load_a.start()

    @pl.when(v < 7)
    def _():
        load_b.start()

    @pl.when(v == 7)
    def _():
        load_c.start()

    zeros[...] = jnp.zeros_like(zeros)
    fills = []
    for r in range(NV):
        lo, hi = 8 * r, min(8 * r + 8, ROWS)
        fills.append(pltpu.make_async_copy(zeros.at[0 : hi - lo, :], blank.at[lo:hi, :], blank_sem.at[r]))
    loads[0].wait()

    sub = lax.broadcasted_iota(jnp.int32, (8, 128), 0)
    lane = lax.broadcasted_iota(jnp.int32, (8, 128), 1)
    marks = mask[...].astype(jnp.float32).astype(jnp.bfloat16)
    i0 = lax.broadcasted_iota(jnp.int32, (128, 128), 0)
    i1 = lax.broadcasted_iota(jnp.int32, (128, 128), 1)
    upto = (i0 <= i1).astype(jnp.float32).astype(jnp.bfloat16)
    before = (i0 < i1).astype(jnp.float32).astype(jnp.bfloat16)
    after = (i0 > i1).astype(jnp.float32).astype(jnp.bfloat16)
    run = jnp.dot(marks, upto, preferred_element_type=jnp.float32).astype(jnp.int32)
    in_lanes = lax.dot_general(
        jnp.ones((8, 128), jnp.bfloat16), marks, (((1,), (1,)), ((), ())), preferred_element_type=jnp.float32
    )
    base = jnp.dot(in_lanes.astype(jnp.bfloat16), before, preferred_element_type=jnp.float32)
    end = base + in_lanes
    tab[...] = jnp.where(sub == 0, base, end).astype(jnp.int32)
    to_smem = pltpu.make_async_copy(tab, stab, sem.at[2])
    to_smem.start()
    total = jnp.sum(in_lanes, axis=1, keepdims=True)
    count[...] = jnp.broadcast_to(total, (8, 128)).astype(jnp.int32)

    in_row = jnp.dot(marks, jnp.ones((128, 128), jnp.bfloat16), preferred_element_type=jnp.float32)
    row_base = jnp.dot(after, in_row.astype(jnp.bfloat16), preferred_element_type=jnp.float32).astype(jnp.int32)
    e = jnp.where(mask[...] > 0, i1 + 128 + ((i1 - run + 1) << 8), 0)
    for bit in range(7):
        far = pltpu.roll(e, 128 - (1 << bit), axis=1)
        comes = (far & (256 << bit)) != 0
        goes = (e & (256 << bit)) != 0
        e = jnp.where(comes, far, jnp.where(goes, 0, e))
    e = e & 255
    turn = row_base & 127
    for bit in range(7):
        e = jnp.where((turn & (1 << bit)) != 0, pltpu.roll(e, 1 << bit, axis=1), e)
    picks[...] = e | jnp.where(i1 < turn, 256, 0)

    for load in loads[1:]:
        load.wait()
    for fill in fills:
        fill.start()

    def step(c, _):
        s = pl.ds(pl.multiple_of(c * 1024, 1024), 1024)

        def row(ref, *at):
            return ref[at[:-1] + (slice(at[-1], at[-1] + 1), s)].reshape(8, 128)

        m = [row(means, i) for i in range(3)]
        sc = [row(scales, i) for i in range(3)]
        q = [row(quats, i) for i in range(4)]
        inv = 1.0 / jnp.sqrt(q[0] * q[0] + q[1] * q[1] + q[2] * q[2] + q[3] * q[3] + 0.25)
        w, xq, y, z = (t * inv for t in q)
        rq = [
            [1 - 2 * (y * y + z * z), 2 * (xq * y - w * z), 2 * (xq * z + w * y)],
            [2 * (xq * y + w * z), 1 - 2 * (xq * xq + z * z), 2 * (y * z - w * xq)],
            [2 * (xq * z - w * y), 2 * (y * z + w * xq), 1 - 2 * (xq * xq + y * y)],
        ]
        factor = [[rq[i][j] * sc[j] for j in range(3)] for i in range(3)]
        gbest = jnp.zeros((8, 128), jnp.float32)
        lbest = jnp.zeros((8, 128), jnp.float32)
        for n in range(seen.shape[0]):
            r = [[rot[i, n, j] for j in range(3)] for i in range(3)]
            p = [r[i][0] * m[0] + r[i][1] * m[1] + r[i][2] * m[2] + trans[n, i] for i in range(3)]
            near = 1.0 / jnp.maximum(p[2], 1.0)
            j00 = focal[n] * near
            j02 = -j00 * p[0] * near
            j12 = -j00 * p[1] * near
            first = [j00 * r[0][j] + j02 * r[2][j] for j in range(3)]
            second = [j00 * r[1][j] + j12 * r[2][j] for j in range(3)]
            pr = [sum(first[j] * factor[j][k] for j in range(3)) for k in range(3)]
            qr = [sum(second[j] * factor[j][k] for j in range(3)) for k in range(3)]
            a = pr[0] * pr[0] + pr[1] * pr[1] + pr[2] * pr[2] + 0.3
            cc = qr[0] * qr[0] + qr[1] * qr[1] + qr[2] * qr[2] + 0.3
            b = pr[0] * qr[0] + pr[1] * qr[1] + pr[2] * qr[2]
            half = 0.5 * (a - cc)
            lam = 0.5 * (a + cc) + jnp.sqrt(half * half + b * b + 0.01)
            on = row(seen, n) > 0
            g0, g1 = row(grad, n, 0), row(grad, n, 1)
            gbest = jnp.maximum(gbest, jnp.where(on, g0 * g0 + g1 * g1, 0.0))
            lbest = jnp.maximum(lbest, jnp.where(on, lam, 0.0))
        piece, at = c // 2, pl.multiple_of((c % 2) * 8, 8)
        part[piece, 0, pl.ds(at, 8), :] = gbest
        part[piece, 1, pl.ds(at, 8), :] = lbest
        gl[0:1, s] = gbest.reshape(1, 1024)
        gl[1:2, s] = lbest.reshape(1, 1024)
        return 0

    lax.fori_loop(0, 16, step, 0)

    load_a.wait()

    @pl.when(v < 7)
    def _():
        load_b.wait()

    @pl.when(v == 7)
    def _():
        load_c.wait()

    @pl.when(v == 0)
    def _():
        x[0:3, :] = means[...]
        x[3:6, :] = scales[...]
        x[6:8, :] = quats[0:2, :]

    @pl.when(v == 1)
    def _():
        x[0:2, :] = quats[2:4, :]
        x[2:8, :] = xb[0:6, :]

    @pl.when((v > 1) & (v < 7))
    def _():
        x[0:2, :] = xa[6:8, :]
        x[2:8, :] = xb[0:6, :]

    @pl.when(v == 7)
    def _():
        x[0:2, :] = xa[6:8, :]
        x[2:3, :] = xb[0:1, :]
        x[3:8, :] = jnp.zeros((5, G), jnp.float32)

    to_smem.wait()

    def pack(c, carry):
        block = stab[0, c] >> 7
        full = (stab[1, c] >> 7) > block
        cols = pl.ds(pl.multiple_of(c * 128, 128), 128)
        pick = jnp.broadcast_to(picks[pl.ds(c, 1), :], (8, 128))
        at, kind = pick & 127, pick & 384
        here, later = kind == 128, kind == 384
        done = []
        for ref, old in zip((x, gl), carry):
            got = jnp.take_along_axis(ref[:, cols], at, axis=1, mode="promise_in_bounds")
            now = jnp.where(here, got, old)
            done.append((now, jnp.where(full, jnp.where(later, got, 0.0), now)))
        tiles[block] = done[0][0]
        packed[block] = done[1][0][0:2]
        return done[0][1], done[1][1]

    zero = jnp.zeros((8, 128), jnp.float32)
    left = lax.fori_loop(0, 128, pack, (zero, zero), unroll=8)
    last = stab[1, 127]

    @pl.when(last < G)
    def _():
        tiles[last >> 7] = left[0]
        packed[last >> 7] = left[1][0:2]

    for fill in fills:
        fill.wait()


def move_kernel(
    part, packed, tiles, count,
    mine, top, best, counts, table, kind,
    taken, takenp, merged, mergedp, turned, turnedp, tab, stab,
    s_part, r_part, s_pack, r_pack, s_best, r_best, s_count, r_count, s_pair, r_pair, s_top, r_top,
    own,
):
    v, g = lax.axis_index("view"), lax.axis_index("gauss")
    gy, gz = g // 8, g % 8
    barrier = pltpu.get_barrier_semaphore()
    each(1, NV, lambda i: pl.semaphore_signal(barrier, inc=1, device_id={"view": (v + i) % NV}, device_id_type=MESH))
    each(1, NG, lambda i: pl.semaphore_signal(barrier, inc=1, device_id={"gauss": (g + i) % NG}, device_id_type=MESH))
    pl.semaphore_wait(barrier, NV - 1 + NG - 1)

    def over_view(peer, src, dst, s, r):
        return pltpu.make_async_remote_copy(src, dst, s, r, device_id={"view": peer}, device_id_type=MESH)

    def over_gauss(peer, src, dst, s, r):
        return pltpu.make_async_remote_copy(src, dst, s, r, device_id={"gauss": peer}, device_id_type=MESH)

    def owner(i):
        return ((gy + i // 8) % 4) * 8 + (gz + i % 8) % 8

    def tell(i, slot):
        return over_gauss((g + i) % NG, count, counts.at[slot], s_count.at[i], r_count.at[slot])

    def give_part(i, slot):
        peer = (v + i) % NV
        return over_view(peer, part.at[peer], taken.at[slot], s_part.at[i], r_part.at[slot])

    def give_best(i, slot):
        return over_view((v + i) % NV, merged, best.at[slot], s_best.at[i], r_best.at[slot])

    def give_pack(i, slot):
        peer = (v + i) % NV
        return over_view(peer, turnedp.at[pl.ds(peer * 16, 16)], takenp.at[slot], s_pack.at[i], r_pack.at[slot])

    def give_top(t):
        at = pl.ds(t * PER, PER)
        return over_gauss(owner(v * 4 + t), mergedp.at[at], top.at[at], s_top.at[t], r_top.at[t])

    each(1, NG, lambda i: tell(i, g).start())
    each(1, NV, lambda i: give_part(i, v).start())
    counts[g] = count[...]
    each(1, NG, lambda i: tell(i, (g + i) % NG).wait_recv())

    def add(s, mine):
        return mine + jnp.where(s < g, (counts[s] + (BLK - 1)) >> 7, 0)

    tab[...] = lax.fori_loop(0, NG, add, jnp.zeros((8, 128), jnp.int32))
    to_smem = pltpu.make_async_copy(tab, stab, own.at[0])
    to_smem.start()
    to_smem.wait()
    shift = stab[0, 0]

    def pair(i):
        at = pl.ds(i * PER, PER)
        return over_gauss(owner(i), turned.at[at], mine.at[at], s_pair.at[i], r_pair.at[i])

    keep = pltpu.make_async_copy(turned.at[0:PER], mine.at[0:PER], own.at[1])

    def turn(i):
        block = (owner(i) - shift) & (NG - 1)
        for w in range(PER):
            turned[i * PER + w] = tiles[block + w * NG]
            turnedp[i * PER + w] = packed[block + w * NG]

    each(0, NG, turn)
    each(1, NG, lambda i: pair(i).start())
    keep.start()
    each(1, NV, lambda i: give_pack(i, v).start())

    def first():
        each(1, NV, lambda i: give_part(i, (v + i) % NV).wait_recv())
        so_far = lax.fori_loop(1, NV, lambda i, so: jnp.maximum(so, taken[(v + i) % NV]), part[v])
        merged[...] = so_far
        best[v] = so_far
        each(1, NV, lambda i: give_best(i, v).start())

    def second():
        each(1, NV, lambda i: give_pack(i, (v + i) % NV).wait_recv())
        best_p = lax.fori_loop(1, NV, lambda i, so: jnp.maximum(so, takenp[(v + i) % NV]), turnedp[pl.ds(v * 16, 16)])
        mergedp[...] = best_p

        @pl.when(v > 0)
        def _():
            give_top(0).start()

        @pl.when(v == 0)
        def _():
            top[0:PER] = best_p[0:PER]

        each(1, 4, lambda t: give_top(t).start())

    def third():
        @pl.when(v > 0)
        def _():
            give_top(0).wait_recv()

        each(1, 4, lambda t: give_top(t).wait_recv())

    first()

    sub = lax.broadcasted_iota(jnp.int32, (8, 128), 0)
    k = lax.broadcasted_iota(jnp.int32, (8, 128), 1) * NG + g
    off = jnp.zeros((8, 128), jnp.int32)
    every = jnp.zeros((8, 128), jnp.int32)
    source = jnp.zeros((8, 128), jnp.int32)
    for s in range(NG):
        n = counts[s]
        blocks = (n + (BLK - 1)) >> 7
        where = (((gy - s // 8) & 3) * 8 + ((gz - s % 8) & 7)) * PER
        inside = (k >= off) & (k < off + blocks)
        source = jnp.where(inside, where + ((k - off) >> 5), source)
        off = off + blocks
        every = every + n
    slots = (off - g + (NG - 1)) >> 5
    most = (off + (NG - 1)) >> 5
    pick = sum((most > size).astype(jnp.int32) for size in SIZES[:-1])
    table[...] = jnp.where(sub == 0, source, jnp.where(sub == 1, every, slots))
    tab[...] = pick
    pick_smem = pltpu.make_async_copy(tab, stab, own.at[0])
    pick_smem.start()

    second()
    third()
    pick_smem.wait()
    kind[0, 0] = stab[0, 0]
    keep.wait()
    each(1, NG, lambda i: pair(i).wait_recv())
    each(1, NV, lambda i: give_best(i, (v + i) % NV).wait_recv())

    each(1, NG, lambda i: tell(i, g).wait_send())
    each(1, NG, lambda i: pair(i).wait_send())
    each(1, NV, lambda i: give_part(i, v).wait_send())
    each(1, NV, lambda i: give_pack(i, v).wait_send())
    each(1, NV, lambda i: give_best(i, v).wait_send())

    @pl.when(v > 0)
    def _():
        give_top(0).wait_send()

    each(1, 4, lambda t: give_top(t).wait_send())


def share_kernel(size, mine, table, top, out, peaks, s_own, r_own, s_side, r_side, s_far, r_far, s_peak, r_peak, own):
    v = lax.axis_index("view")
    core, chip = v % 2, v // 2
    mate = chip * 2 + 1 - core
    right, left, far = (((chip + i) % 4) * 2 + core for i in (1, 3, 2))
    barrier = pltpu.get_barrier_semaphore()
    each(1, NV, lambda i: pl.semaphore_signal(barrier, inc=1, device_id={"view": (v + i) % NV}, device_id_type=MESH))
    rows = pl.ds(pl.multiple_of(v * 8, 8), 8)

    def cols(at):
        return pl.ds(pl.multiple_of(at * BLK, BLK), BLK)

    def place(q):
        out[rows, cols(q)] = mine[table[0, q]]

    each(0, size, place)
    keep = pltpu.make_async_copy(top, peaks.at[pl.ds(v * 16, 16)], own.at[0])
    keep.start()
    pl.semaphore_wait(barrier, NV - 1)
    wide = size * BLK // CHUNKS

    def over_view(peer, group, c, s, r):
        at = out.at[pl.ds(pl.multiple_of(group * 8, 8), 8), c * wide : (c + 1) * wide]
        return pltpu.make_async_remote_copy(at, at, s, r, device_id={"view": peer}, device_id_type=MESH)

    def side(kind, c, group):
        return over_view(mate, group, c, s_side.at[kind, c], r_side.at[kind, c])

    def go(way, c, group):
        return over_view(right if way == 0 else left, group, c, s_own.at[way, c], r_own.at[way, c])

    def on(way, c, group):
        return over_view(right if way == 0 else left, group, c, s_far.at[c], r_far.at[c])

    for c in range(CHUNKS):
        go(0, c, v).start()
        go(1, c, v).start()
        side(0, c, v).start()
    def give_peak(i, slot):
        return pltpu.make_async_remote_copy(
            top,
            peaks.at[pl.ds(slot * 16, 16)],
            s_peak.at[i],
            r_peak.at[slot],
            device_id={"view": (v + i) % NV},
            device_id_type=MESH,
        )

    each(1, NV, lambda i: give_peak(i, v).start())
    for c in range(CHUNKS):
        go(0, c, left).wait_recv()
        if c < CHUNKS // 2:
            on(0, c, left).start()
        side(2, c, left).start()
        go(1, c, right).wait_recv()
        if c >= CHUNKS // 2:
            on(1, c, right).start()
        side(1, c, right).start()
    for c in range(CHUNKS):
        on(0, c, far).wait_recv()
        side(3, c, far).start()
    across = [mate, right + 1 - 2 * core, left + 1 - 2 * core, far + 1 - 2 * core]
    for c in range(CHUNKS):
        for kind in range(4):
            side(kind, c, across[kind]).wait_recv()
            side(kind, c, v).wait_send()
        go(0, c, v).wait_send()
        go(1, c, v).wait_send()
        on(0, c, v).wait_send()
    each(1, NV, lambda i: give_peak(i, (v + i) % NV).wait_recv())
    each(1, NV, lambda i: give_peak(i, v).wait_send())
    keep.wait()


def lay_kernel(size, table, best, peaks, tiles, blank, clones, peak, total, stage, sem):
    del blank
    sub = lax.broadcasted_iota(jnp.int32, (8, 128), 0)
    used = table[2, 0]
    total[0, 0] = table[1, 0]

    def cols(at):
        return pl.ds(pl.multiple_of(at * BLK, BLK), BLK)

    def copies(src, dst, sem):
        for n in (128, 64, 32, 16, 8, 4, 2, 1):
            at = pl.ds(pl.multiple_of((used & (256 - 2 * n)) * BLK, BLK), n * BLK)
            if n <= size:
                yield (used & n) != 0, pltpu.make_async_copy(src.at[:, at], dst.at[:, at], sem)

    main = list(copies(tiles.at[0:56, :], clones.at[0:56, :], sem.at[0]))
    rest = list(copies(stage.at[0 : ROWS - 56, :], clones.at[56:ROWS, :], sem.at[1]))
    for on, copy in main:
        pl.when(on)(copy.start)

    def finish(q):
        tops = peaks[table[0, q]]
        gtop = jnp.broadcast_to(jnp.sqrt(tops[0:1]), (8, 128))
        ltop = jnp.broadcast_to(3.0 * jnp.sqrt(tops[1:2]), (8, 128))
        tile = tiles[56:64, cols(q)]
        stage[:, cols(q)] = jnp.where(sub == 3, gtop, jnp.where(sub == 4, ltop, tile))

    each(0, used, finish)
    for on, copy in rest:
        pl.when(on)(copy.start)

    def roots(c, _):
        s = pl.ds(pl.multiple_of(c * 1024, 1024), 1024)
        piece, at = c // 2, pl.multiple_of((c % 2) * 8, 8)
        peak[0:1, s] = jnp.sqrt(best[piece, 0, pl.ds(at, 8), :]).reshape(1, 1024)
        peak[1:2, s] = (3.0 * jnp.sqrt(best[piece, 1, pl.ds(at, 8), :])).reshape(1, 1024)
        return 0

    lax.fori_loop(0, 16, roots, 0)
    for on, copy in main + rest:
        pl.when(on)(copy.wait)


def body(means, scales, quats, attrs, grad_screen, visible, clone_mask, rotation, shift, focal):
    f32, i32 = jnp.float32, jnp.int32
    shape = jax.ShapeDtypeStruct
    dma = pltpu.SemaphoreType.DMA
    mask = clone_mask.reshape(128, 128)
    part, packed, tiles, count, blank = pl.pallas_call(
        front_kernel,
        in_specs=[HBM] * 10,
        out_specs=(VMEM,) * 4 + (HBM,),
        out_shape=(
            shape((NV, 2, 16, 128), f32),
            shape((CAP, 2, 128), f32),
            shape((CAP, 8, 128), f32),
            shape((8, 128), i32),
            shape((ROWS, G), f32),
        ),
        scratch_shapes=[
            pltpu.VMEM((128, 128), i32),
            pltpu.VMEM((3, G), f32),
            pltpu.VMEM((3, G), f32),
            pltpu.VMEM((4, G), f32),
            pltpu.VMEM((4, 2, G), f32),
            pltpu.VMEM((4, G), i32),
            pltpu.SMEM((3, 4, 3), f32),
            pltpu.SMEM((4, 3), f32),
            pltpu.SMEM((4,), f32),
            pltpu.VMEM((8, G), f32),
            pltpu.VMEM((8, G), f32),
            pltpu.VMEM((8, G), f32),
            pltpu.VMEM((8, G), f32),
            pltpu.VMEM((128, 128), i32),
            pltpu.VMEM((8, 128), i32),
            pltpu.SMEM((8, 128), i32),
            pltpu.VMEM((8, G), f32),
            dma((3,)),
            dma((9,)),
            dma((NV,)),
        ],
        compiler_params=pltpu.CompilerParams(vmem_limit_bytes=16 * 2**20),
        name="front",
    )(
        *(
            pltpu.with_memory_space_constraint(a, pltpu.HBM)
            for a in (mask, means, scales, quats, grad_screen, visible, rotation.transpose(1, 0, 2), shift, focal, attrs)
        )
    )

    mine, top, best, _, table, kind = pl.pallas_call(
        move_kernel,
        in_specs=[VMEM] * 4,
        out_specs=(VMEM,) * 5 + (SMEM,),
        out_shape=(
            shape((CAP, 8, 128), f32),
            shape((16, 2, 128), f32),
            shape((NV, 2, 16, 128), f32),
            shape((NG, 8, 128), i32),
            shape((8, 128), i32),
            shape((1, 1), i32),
        ),
        scratch_shapes=[
            pltpu.VMEM((NV, 2, 16, 128), f32),
            pltpu.VMEM((NV, 16, 2, 128), f32),
            pltpu.VMEM((2, 16, 128), f32),
            pltpu.VMEM((16, 2, 128), f32),
            pltpu.VMEM((CAP, 8, 128), f32),
            pltpu.VMEM((CAP, 2, 128), f32),
            pltpu.VMEM((8, 128), i32),
            pltpu.SMEM((8, 128), i32),
        ]
        + [dma((NV,))] * 6
        + [dma((NG,))] * 4
        + [dma((4,))] * 2
        + [dma((2,))],
        compiler_params=pltpu.CompilerParams(
            collective_id=0, has_side_effects=True, vmem_limit_bytes=16 * 2**20
        ),
        name="move",
    )(part, packed, tiles, count)

    def share(n, size):
        gather = pl.pallas_call(
            functools.partial(share_kernel, size),
            in_specs=[VMEM, SMEM, VMEM],
            out_specs=(VMEM, VMEM),
            out_shape=(shape((8 * NV, size * BLK), f32), shape((CAP, 2, 128), f32)),
            scratch_shapes=[dma((2, CHUNKS))] * 2
            + [dma((4, CHUNKS))] * 2
            + [dma((CHUNKS,))] * 2
            + [dma((NV,))] * 2
            + [dma((1,))],
            compiler_params=pltpu.CompilerParams(
                collective_id=1 + n, has_side_effects=True, vmem_limit_bytes=16 * 2**20
            ),
            name=f"share{size}",
        )
        lay = pl.pallas_call(
            functools.partial(lay_kernel, size),
            in_specs=[SMEM, VMEM, VMEM, VMEM, HBM],
            out_specs=(HBM, VMEM, SMEM),
            out_shape=(shape((ROWS, G), f32), shape((2, G), f32), shape((1, 1), i32)),
            input_output_aliases={4: 0},
            scratch_shapes=[pltpu.VMEM((8, size * BLK), f32), dma((2,))],
            compiler_params=pltpu.CompilerParams(vmem_limit_bytes=16 * 2**20),
            name=f"lay{size}",
        )
        def branch(mine, table, best, top, blank):
            tiles, peaks = gather(mine, table, top)
            return lay(table, best, peaks, tiles, pltpu.with_memory_space_constraint(blank, pltpu.HBM))

        return branch

    blank = pltpu.with_memory_space_constraint(blank, pltpu.HBM)
    branches = [share(n, size) for n, size in enumerate(SIZES)]
    clones, peak, total = lax.switch(kind.reshape(()), branches, mine, table, best, top, blank)
    return (peak, clones, total.reshape(()))


def solution(mesh):
    return jax.shard_map(
        body,
        mesh=mesh,
        in_specs=(
            P(None, "gauss"),
            P(None, "gauss"),
            P(None, "gauss"),
            P(None, "gauss"),
            P("view", None, "gauss"),
            P("view", "gauss"),
            P("gauss"),
            P("view", None, None),
            P("view", None),
            P("view"),
        ),
        out_specs=(P(None, "gauss"), P(None, "gauss"), P()),
        check_vma=False,
    )
```

```python
import functools

import jax
import jax.numpy as jnp
from jax import lax
from jax.experimental import pallas as pl
from jax.experimental.pallas import tpu as pltpu
from jax.sharding import PartitionSpec as P

G = 16384
ROWS = 61
BLK = 128
CAP = G // BLK
NV = 8
NG = 32
PER = CAP // NG
CHUNKS = 4
FIRST = 60
MESH = pl.DeviceIdType.MESH
VMEM = pl.BlockSpec(memory_space=pltpu.VMEM)
SMEM = pl.BlockSpec(memory_space=pltpu.SMEM)
HBM = pl.BlockSpec(memory_space=pltpu.HBM)


def each(lo, n, do):
    if isinstance(lo, int) and isinstance(n, int):
        for i in range(lo, n):
            do(i)
        return

    def one(i, _):
        do(i)
        return 0

    lax.fori_loop(lo, n, one, 0)


def front_kernel(
    mask_h, means_h, scales_h, quats_h, grad_h, seen_h, rot_h, trans_h, focal_h, attrs,
    part, packed, tiles, count, blank,
    mask, means, scales, quats, grad, seen, rot, trans, focal,
    xa, xb, x, gl, picks, tab, stab, zeros, sem, load_sem, blank_sem,
):
    v = lax.axis_index("view")
    pairs = (
        (mask_h, mask), (rot_h, rot), (trans_h, trans), (focal_h, focal), (means_h, means), (scales_h, scales),
        (quats_h, quats), (seen_h, seen), (grad_h, grad),
    )
    loads = [pltpu.make_async_copy(src, dst, load_sem.at[i]) for i, (src, dst) in enumerate(pairs)]
    for load in loads:
        load.start()
    a_at = pl.multiple_of(jnp.clip(v - 2, 0, 5) * 8, 8)
    b_at = pl.multiple_of(jnp.clip(v - 1, 0, 5) * 8, 8)
    load_a = pltpu.make_async_copy(attrs.at[pl.ds(a_at, 8), :], xa, sem.at[0])
    load_b = pltpu.make_async_copy(attrs.at[pl.ds(b_at, 8), :], xb, sem.at[1])
    load_c = pltpu.make_async_copy(attrs.at[48:49, :], xb.at[0:1, :], sem.at[1])
    load_a.start()

    @pl.when(v < 7)
    def _():
        load_b.start()

    @pl.when(v == 7)
    def _():
        load_c.start()

    zeros[...] = jnp.zeros_like(zeros)
    fills = []
    for r in range(NV):
        lo, hi = 8 * r, min(8 * r + 8, ROWS)
        fills.append(pltpu.make_async_copy(zeros.at[0 : hi - lo, :], blank.at[lo:hi, :], blank_sem.at[r]))
    loads[0].wait()

    sub = lax.broadcasted_iota(jnp.int32, (8, 128), 0)
    lane = lax.broadcasted_iota(jnp.int32, (8, 128), 1)
    marks = mask[...].astype(jnp.float32).astype(jnp.bfloat16)
    i0 = lax.broadcasted_iota(jnp.int32, (128, 128), 0)
    i1 = lax.broadcasted_iota(jnp.int32, (128, 128), 1)
    upto = (i0 <= i1).astype(jnp.float32).astype(jnp.bfloat16)
    before = (i0 < i1).astype(jnp.float32).astype(jnp.bfloat16)
    after = (i0 > i1).astype(jnp.float32).astype(jnp.bfloat16)
    run = jnp.dot(marks, upto, preferred_element_type=jnp.float32).astype(jnp.int32)
    in_lanes = lax.dot_general(
        jnp.ones((8, 128), jnp.bfloat16), marks, (((1,), (1,)), ((), ())), preferred_element_type=jnp.float32
    )
    base = jnp.dot(in_lanes.astype(jnp.bfloat16), before, preferred_element_type=jnp.float32)
    end = base + in_lanes
    tab[...] = jnp.where(sub == 0, base, end).astype(jnp.int32)
    to_smem = pltpu.make_async_copy(tab, stab, sem.at[2])
    to_smem.start()
    total = jnp.sum(in_lanes, axis=1, keepdims=True)
    count[...] = jnp.broadcast_to(total, (8, 128)).astype(jnp.int32)

    in_row = jnp.dot(marks, jnp.ones((128, 128), jnp.bfloat16), preferred_element_type=jnp.float32)
    row_base = jnp.dot(after, in_row.astype(jnp.bfloat16), preferred_element_type=jnp.float32).astype(jnp.int32)
    e = jnp.where(mask[...] > 0, i1 + 128 + ((i1 - run + 1) << 8), 0)
    for bit in range(7):
        far = pltpu.roll(e, 128 - (1 << bit), axis=1)
        comes = (far & (256 << bit)) != 0
        goes = (e & (256 << bit)) != 0
        e = jnp.where(comes, far, jnp.where(goes, 0, e))
    e = e & 255
    turn = row_base & 127
    for bit in range(7):
        e = jnp.where((turn & (1 << bit)) != 0, pltpu.roll(e, 1 << bit, axis=1), e)
    picks[...] = e | jnp.where(i1 < turn, 256, 0)

    for load in loads[1:]:
        load.wait()
    for fill in fills:
        fill.start()

    def step(c, _):
        s = pl.ds(pl.multiple_of(c * 1024, 1024), 1024)

        def row(ref, *at):
            return ref[at[:-1] + (slice(at[-1], at[-1] + 1), s)].reshape(8, 128)

        m = [row(means, i) for i in range(3)]
        sc = [row(scales, i) for i in range(3)]
        q = [row(quats, i) for i in range(4)]
        inv = 1.0 / jnp.sqrt(q[0] * q[0] + q[1] * q[1] + q[2] * q[2] + q[3] * q[3] + 0.25)
        w, xq, y, z = (t * inv for t in q)
        rq = [
            [1 - 2 * (y * y + z * z), 2 * (xq * y - w * z), 2 * (xq * z + w * y)],
            [2 * (xq * y + w * z), 1 - 2 * (xq * xq + z * z), 2 * (y * z - w * xq)],
            [2 * (xq * z - w * y), 2 * (y * z + w * xq), 1 - 2 * (xq * xq + y * y)],
        ]
        factor = [[rq[i][j] * sc[j] for j in range(3)] for i in range(3)]
        gbest = jnp.zeros((8, 128), jnp.float32)
        lbest = jnp.zeros((8, 128), jnp.float32)
        for n in range(seen.shape[0]):
            r = [[rot[i, n, j] for j in range(3)] for i in range(3)]
            p = [r[i][0] * m[0] + r[i][1] * m[1] + r[i][2] * m[2] + trans[n, i] for i in range(3)]
            near = 1.0 / jnp.maximum(p[2], 1.0)
            j00 = focal[n] * near
            j02 = -j00 * p[0] * near
            j12 = -j00 * p[1] * near
            first = [j00 * r[0][j] + j02 * r[2][j] for j in range(3)]
            second = [j00 * r[1][j] + j12 * r[2][j] for j in range(3)]
            pr = [sum(first[j] * factor[j][k] for j in range(3)) for k in range(3)]
            qr = [sum(second[j] * factor[j][k] for j in range(3)) for k in range(3)]
            a = pr[0] * pr[0] + pr[1] * pr[1] + pr[2] * pr[2] + 0.3
            cc = qr[0] * qr[0] + qr[1] * qr[1] + qr[2] * qr[2] + 0.3
            b = pr[0] * qr[0] + pr[1] * qr[1] + pr[2] * qr[2]
            half = 0.5 * (a - cc)
            lam = 0.5 * (a + cc) + jnp.sqrt(half * half + b * b + 0.01)
            on = row(seen, n) > 0
            g0, g1 = row(grad, n, 0), row(grad, n, 1)
            gbest = jnp.maximum(gbest, jnp.where(on, g0 * g0 + g1 * g1, 0.0))
            lbest = jnp.maximum(lbest, jnp.where(on, lam, 0.0))
        piece, at = c // 2, pl.multiple_of((c % 2) * 8, 8)
        part[piece, 0, pl.ds(at, 8), :] = gbest
        part[piece, 1, pl.ds(at, 8), :] = lbest
        gl[0:1, s] = gbest.reshape(1, 1024)
        gl[1:2, s] = lbest.reshape(1, 1024)
        return 0

    lax.fori_loop(0, 16, step, 0)

    load_a.wait()

    @pl.when(v < 7)
    def _():
        load_b.wait()

    @pl.when(v == 7)
    def _():
        load_c.wait()

    @pl.when(v == 0)
    def _():
        x[0:3, :] = means[...]
        x[3:6, :] = scales[...]
        x[6:8, :] = quats[0:2, :]

    @pl.when(v == 1)
    def _():
        x[0:2, :] = quats[2:4, :]
        x[2:8, :] = xb[0:6, :]

    @pl.when((v > 1) & (v < 7))
    def _():
        x[0:2, :] = xa[6:8, :]
        x[2:8, :] = xb[0:6, :]

    @pl.when(v == 7)
    def _():
        x[0:2, :] = xa[6:8, :]
        x[2:3, :] = xb[0:1, :]
        x[3:8, :] = jnp.zeros((5, G), jnp.float32)

    to_smem.wait()

    def pack(c, carry):
        block = stab[0, c] >> 7
        full = (stab[1, c] >> 7) > block
        cols = pl.ds(pl.multiple_of(c * 128, 128), 128)
        pick = jnp.broadcast_to(picks[pl.ds(c, 1), :], (8, 128))
        at, kind = pick & 127, pick & 384
        here, later = kind == 128, kind == 384
        done = []
        for ref, old in zip((x, gl), carry):
            got = jnp.take_along_axis(ref[:, cols], at, axis=1, mode="promise_in_bounds")
            now = jnp.where(here, got, old)
            done.append((now, jnp.where(full, jnp.where(later, got, 0.0), now)))
        tiles[block] = done[0][0]
        packed[block] = done[1][0][0:2]
        return done[0][1], done[1][1]

    zero = jnp.zeros((8, 128), jnp.float32)
    left = lax.fori_loop(0, 128, pack, (zero, zero), unroll=8)
    last = stab[1, 127]

    @pl.when(last < G)
    def _():
        tiles[last >> 7] = left[0]
        packed[last >> 7] = left[1][0:2]

    for fill in fills:
        fill.wait()


def spread(out, size, source, mine, s_own, r_own, s_side, r_side, s_far, r_far, ready):
    v = lax.axis_index("view")
    core, chip = v % 2, v // 2
    mate = chip * 2 + 1 - core
    right, left, far = (((chip + i) % 4) * 2 + core for i in (1, 3, 2))
    rows = pl.ds(pl.multiple_of(v * 8, 8), 8)

    def place(q, _):
        out[rows, pl.ds(pl.multiple_of(q * BLK, BLK), BLK)] = mine[source(q)]
        return 0

    lax.fori_loop(0, size, place, 0, unroll=4)
    ready()
    wide = size * BLK // CHUNKS

    def over_view(peer, group, c, s, r):
        at = out.at[pl.ds(pl.multiple_of(group * 8, 8), 8), c * wide : (c + 1) * wide]
        return pltpu.make_async_remote_copy(at, at, s, r, device_id={"view": peer}, device_id_type=MESH)

    def side(kind, c, group):
        return over_view(mate, group, c, s_side.at[kind, c], r_side.at[kind, c])

    def go(way, c, group):
        return over_view(right if way == 0 else left, group, c, s_own.at[way, c], r_own.at[way, c])

    def on(way, c, group):
        return over_view(right if way == 0 else left, group, c, s_far.at[c], r_far.at[c])

    for c in range(CHUNKS):
        go(0, c, v).start()
        go(1, c, v).start()
        side(0, c, v).start()
    for c in range(CHUNKS):
        go(0, c, left).wait_recv()
        if c < CHUNKS // 2:
            on(0, c, left).start()
        side(2, c, left).start()
        go(1, c, right).wait_recv()
        if c >= CHUNKS // 2:
            on(1, c, right).start()
        side(1, c, right).start()
    for c in range(CHUNKS):
        on(0, c, far).wait_recv()
        side(3, c, far).start()
    across = [mate, right + 1 - 2 * core, left + 1 - 2 * core, far + 1 - 2 * core]
    for c in range(CHUNKS):
        for kind in range(4):
            side(kind, c, across[kind]).wait_recv()
            side(kind, c, v).wait_send()
        go(0, c, v).wait_send()
        go(1, c, v).wait_send()
        on(0, c, v).wait_send()


def move_kernel(
    part, packed, tiles, count,
    mine, out, peaks, best, counts, table, kind,
    taken, takenp, merged, mergedp, top, turned, turnedp, tab, stab,
    s_part, r_part, s_pack, r_pack, s_best, r_best, s_peak, r_peak, s_count, r_count, s_pair, r_pair, s_top, r_top,
    s_own, r_own, s_side, r_side, s_far, r_far, own,
):
    v, g = lax.axis_index("view"), lax.axis_index("gauss")
    gy, gz = g // 8, g % 8
    barrier = pltpu.get_barrier_semaphore()
    each(1, NV, lambda i: pl.semaphore_signal(barrier, inc=1, device_id={"view": (v + i) % NV}, device_id_type=MESH))
    each(1, NG, lambda i: pl.semaphore_signal(barrier, inc=1, device_id={"gauss": (g + i) % NG}, device_id_type=MESH))
    pl.semaphore_wait(barrier, NV - 1 + NG - 1)

    def over_view(peer, src, dst, s, r):
        return pltpu.make_async_remote_copy(src, dst, s, r, device_id={"view": peer}, device_id_type=MESH)

    def over_gauss(peer, src, dst, s, r):
        return pltpu.make_async_remote_copy(src, dst, s, r, device_id={"gauss": peer}, device_id_type=MESH)

    def owner(i):
        return ((gy + i // 8) % 4) * 8 + (gz + i % 8) % 8

    def tell(i, slot):
        return over_gauss((g + i) % NG, count, counts.at[slot], s_count.at[i], r_count.at[slot])

    def give_part(i, slot):
        peer = (v + i) % NV
        return over_view(peer, part.at[peer], taken.at[slot], s_part.at[i], r_part.at[slot])

    def give_best(i, slot):
        return over_view((v + i) % NV, merged, best.at[slot], s_best.at[i], r_best.at[slot])

    def give_pack(i, slot):
        peer = (v + i) % NV
        return over_view(peer, turnedp.at[pl.ds(peer * 16, 16)], takenp.at[slot], s_pack.at[i], r_pack.at[slot])

    def give_top(t):
        at = pl.ds(t * PER, PER)
        return over_gauss(owner(v * 4 + t), mergedp.at[at], top.at[at], s_top.at[t], r_top.at[t])

    each(1, NG, lambda i: tell(i, g).start())
    each(1, NV, lambda i: give_part(i, v).start())
    counts[g] = count[...]
    each(1, NG, lambda i: tell(i, (g + i) % NG).wait_recv())

    def add(s, mine):
        return mine + jnp.where(s < g, (counts[s] + (BLK - 1)) >> 7, 0)

    tab[...] = lax.fori_loop(0, NG, add, jnp.zeros((8, 128), jnp.int32))
    to_smem = pltpu.make_async_copy(tab, stab, own.at[0])
    to_smem.start()
    to_smem.wait()
    shift = stab[0, 0]

    def pair(i):
        at = pl.ds(i * PER, PER)
        return over_gauss(owner(i), turned.at[at], mine.at[at], s_pair.at[i], r_pair.at[i])

    keep = pltpu.make_async_copy(turned.at[0:PER], mine.at[0:PER], own.at[1])

    def turn(i):
        block = (owner(i) - shift) & (NG - 1)
        for w in range(PER):
            turned[i * PER + w] = tiles[block + w * NG]
            turnedp[i * PER + w] = packed[block + w * NG]

    each(0, NG, turn)
    each(1, NG, lambda i: pair(i).start())
    keep.start()
    each(1, NV, lambda i: give_pack(i, v).start())

    def first():
        each(1, NV, lambda i: give_part(i, (v + i) % NV).wait_recv())
        so_far = lax.fori_loop(1, NV, lambda i, so: jnp.maximum(so, taken[(v + i) % NV]), part[v])
        merged[...] = so_far
        best[v] = so_far
        each(1, NV, lambda i: give_best(i, v).start())

    def second():
        each(1, NV, lambda i: give_pack(i, (v + i) % NV).wait_recv())
        best_p = lax.fori_loop(1, NV, lambda i, so: jnp.maximum(so, takenp[(v + i) % NV]), turnedp[pl.ds(v * 16, 16)])
        mergedp[...] = best_p

        @pl.when(v > 0)
        def _():
            give_top(0).start()

        @pl.when(v == 0)
        def _():
            top[0:PER] = best_p[0:PER]

        each(1, 4, lambda t: give_top(t).start())

    def third():
        @pl.when(v > 0)
        def _():
            give_top(0).wait_recv()

        each(1, 4, lambda t: give_top(t).wait_recv())

    first()

    sub = lax.broadcasted_iota(jnp.int32, (8, 128), 0)
    k = lax.broadcasted_iota(jnp.int32, (8, 128), 1) * NG + g
    off = jnp.zeros((8, 128), jnp.int32)
    every = jnp.zeros((8, 128), jnp.int32)
    source = jnp.zeros((8, 128), jnp.int32)
    for s in range(NG):
        n = counts[s]
        blocks = (n + (BLK - 1)) >> 7
        where = (((gy - s // 8) & 3) * 8 + ((gz - s % 8) & 7)) * PER
        inside = (k >= off) & (k < off + blocks)
        source = jnp.where(inside, where + ((k - off) >> 5), source)
        off = off + blocks
        every = every + n
    slots = (off - g + (NG - 1)) >> 5
    most = (off + (NG - 1)) >> 5
    more = (most > FIRST).astype(jnp.int32)
    filled = jnp.where(sub == 0, source, jnp.where(sub == 1, every, jnp.where(sub == 2, slots, more)))
    table[...] = filled
    tab[...] = filled
    pick_smem = pltpu.make_async_copy(tab, stab, own.at[0])
    pick_smem.start()

    second()
    third()
    pick_smem.wait()
    kind[0, 0] = stab[3, 0]

    def give_peak(i, slot):
        at = peaks.at[pl.ds(slot * 16, 16)]
        return over_view((v + i) % NV, top, at, s_peak.at[i], r_peak.at[slot])

    each(1, NV, lambda i: give_peak(i, v).start())
    peaks[pl.ds(v * 16, 16)] = top[...]
    keep.wait()
    each(1, NG, lambda i: pair(i).wait_recv())
    spread(
        out, FIRST, lambda q: stab[0, q], mine, s_own, r_own, s_side, r_side, s_far, r_far, lambda: None
    )
    each(1, NV, lambda i: give_peak(i, (v + i) % NV).wait_recv())
    each(1, NV, lambda i: give_peak(i, v).wait_send())
    each(1, NV, lambda i: give_best(i, (v + i) % NV).wait_recv())

    each(1, NG, lambda i: tell(i, g).wait_send())
    each(1, NG, lambda i: pair(i).wait_send())
    each(1, NV, lambda i: give_part(i, v).wait_send())
    each(1, NV, lambda i: give_pack(i, v).wait_send())
    each(1, NV, lambda i: give_best(i, v).wait_send())

    @pl.when(v > 0)
    def _():
        give_top(0).wait_send()

    each(1, 4, lambda t: give_top(t).wait_send())


def share_kernel(mine, table, out, *sems):
    v = lax.axis_index("view")
    barrier = pltpu.get_barrier_semaphore()
    each(1, NV, lambda i: pl.semaphore_signal(barrier, inc=1, device_id={"view": (v + i) % NV}, device_id_type=MESH))
    spread(out, CAP - FIRST, lambda q: table[0, FIRST + q], mine, *sems, lambda: pl.semaphore_wait(barrier, NV - 1))


def lay_kernel(more, table, best, peaks, tiles, *refs):
    rest, _, clones, peak, total, stage, sem = refs if more else (None, *refs)
    sub = lax.broadcasted_iota(jnp.int32, (8, 128), 0)
    used = table[2, 0]
    total[0, 0] = table[1, 0]

    def cols(at):
        return pl.ds(pl.multiple_of(at * BLK, BLK), BLK)

    def runs(count, most):
        for n in (64, 32, 16, 8, 4, 2, 1):
            if n <= most:
                yield (count & n) != 0, pl.multiple_of((count & (256 - 2 * n)) * BLK, BLK), n * BLK

    if more:
        pieces = [(tiles, 0, (True, 0, FIRST * BLK))]
        pieces += [(rest, FIRST, run) for run in runs(used - FIRST, CAP - FIRST)]
    else:
        pieces = [(tiles, 0, run) for run in runs(used, FIRST)]
    main, last = [], []
    for src, first, (on, at, size) in pieces:
        to = pl.multiple_of(at + first * BLK, BLK)
        main.append((on, pltpu.make_async_copy(
            src.at[0:56, pl.ds(at, size)], clones.at[0:56, pl.ds(to, size)], sem.at[0]
        )))
        last.append((on, pltpu.make_async_copy(
            stage.at[0 : ROWS - 56, pl.ds(to, size)], clones.at[56:ROWS, pl.ds(to, size)], sem.at[1]
        )))
    for on, copy in main:
        pl.when(on)(copy.start)

    def finish(src, first):
        def one(q):
            tops = peaks[table[0, q]]
            gtop = jnp.broadcast_to(jnp.sqrt(tops[0:1]), (8, 128))
            ltop = jnp.broadcast_to(3.0 * jnp.sqrt(tops[1:2]), (8, 128))
            tile = src[56:64, cols(q - first)]
            stage[:, cols(q)] = jnp.where(sub == 3, gtop, jnp.where(sub == 4, ltop, tile))

        return one

    each(jnp.int32(0), jnp.minimum(used, FIRST), finish(tiles, 0))
    if more:
        each(jnp.int32(FIRST), used, finish(rest, FIRST))
    for on, copy in last:
        pl.when(on)(copy.start)

    def roots(c, _):
        s = pl.ds(pl.multiple_of(c * 1024, 1024), 1024)
        piece, at = c // 2, pl.multiple_of((c % 2) * 8, 8)
        peak[0:1, s] = jnp.sqrt(best[piece, 0, pl.ds(at, 8), :]).reshape(1, 1024)
        peak[1:2, s] = (3.0 * jnp.sqrt(best[piece, 1, pl.ds(at, 8), :])).reshape(1, 1024)
        return 0

    lax.fori_loop(0, 16, roots, 0)
    for on, copy in main + last:
        pl.when(on)(copy.wait)


def body(means, scales, quats, attrs, grad_screen, visible, clone_mask, rotation, shift, focal):
    f32, i32 = jnp.float32, jnp.int32
    shape = jax.ShapeDtypeStruct
    dma = pltpu.SemaphoreType.DMA
    view_sems = [dma((2, CHUNKS))] * 2 + [dma((4, CHUNKS))] * 2 + [dma((CHUNKS,))] * 2
    mask = clone_mask.reshape(128, 128)
    part, packed, tiles, count, blank = pl.pallas_call(
        front_kernel,
        in_specs=[HBM] * 10,
        out_specs=(VMEM,) * 4 + (HBM,),
        out_shape=(
            shape((NV, 2, 16, 128), f32),
            shape((CAP, 2, 128), f32),
            shape((CAP, 8, 128), f32),
            shape((8, 128), i32),
            shape((ROWS, G), f32),
        ),
        scratch_shapes=[
            pltpu.VMEM((128, 128), i32),
            pltpu.VMEM((3, G), f32),
            pltpu.VMEM((3, G), f32),
            pltpu.VMEM((4, G), f32),
            pltpu.VMEM((4, 2, G), f32),
            pltpu.VMEM((4, G), i32),
            pltpu.SMEM((3, 4, 3), f32),
            pltpu.SMEM((4, 3), f32),
            pltpu.SMEM((4,), f32),
            pltpu.VMEM((8, G), f32),
            pltpu.VMEM((8, G), f32),
            pltpu.VMEM((8, G), f32),
            pltpu.VMEM((8, G), f32),
            pltpu.VMEM((128, 128), i32),
            pltpu.VMEM((8, 128), i32),
            pltpu.SMEM((8, 128), i32),
            pltpu.VMEM((8, G), f32),
            dma((3,)),
            dma((9,)),
            dma((NV,)),
        ],
        compiler_params=pltpu.CompilerParams(vmem_limit_bytes=16 * 2**20),
        name="front",
    )(
        *(
            pltpu.with_memory_space_constraint(a, pltpu.HBM)
            for a in (mask, means, scales, quats, grad_screen, visible, rotation.transpose(1, 0, 2), shift, focal, attrs)
        )
    )

    mine, out, peaks, best, _, table, kind = pl.pallas_call(
        move_kernel,
        in_specs=[VMEM] * 4,
        out_specs=(VMEM,) * 6 + (SMEM,),
        out_shape=(
            shape((CAP, 8, 128), f32),
            shape((8 * NV, FIRST * BLK), f32),
            shape((CAP, 2, 128), f32),
            shape((NV, 2, 16, 128), f32),
            shape((NG, 8, 128), i32),
            shape((8, 128), i32),
            shape((1, 1), i32),
        ),
        scratch_shapes=[
            pltpu.VMEM((NV, 2, 16, 128), f32),
            pltpu.VMEM((NV, 16, 2, 128), f32),
            pltpu.VMEM((2, 16, 128), f32),
            pltpu.VMEM((16, 2, 128), f32),
            pltpu.VMEM((16, 2, 128), f32),
            pltpu.VMEM((CAP, 8, 128), f32),
            pltpu.VMEM((CAP, 2, 128), f32),
            pltpu.VMEM((8, 128), i32),
            pltpu.SMEM((8, 128), i32),
        ]
        + [dma((NV,))] * 8
        + [dma((NG,))] * 4
        + [dma((4,))] * 2
        + view_sems
        + [dma((2,))],
        compiler_params=pltpu.CompilerParams(
            collective_id=0, has_side_effects=True, vmem_limit_bytes=16 * 2**20
        ),
        name="move",
    )(part, packed, tiles, count)

    share = pl.pallas_call(
        share_kernel,
        in_specs=[VMEM, SMEM],
        out_specs=VMEM,
        out_shape=shape((8 * NV, (CAP - FIRST) * BLK), f32),
        scratch_shapes=view_sems,
        compiler_params=pltpu.CompilerParams(
            collective_id=1, has_side_effects=True, vmem_limit_bytes=16 * 2**20
        ),
        name="share",
    )

    def lay(more, table, best, peaks, *tiles_and_blank):
        return pl.pallas_call(
            functools.partial(lay_kernel, more),
            in_specs=[SMEM, VMEM, VMEM] + [VMEM] * (1 + more) + [HBM],
            out_specs=(HBM, VMEM, SMEM),
            out_shape=(shape((ROWS, G), f32), shape((2, G), f32), shape((1, 1), i32)),
            input_output_aliases={4 + more: 0},
            scratch_shapes=[pltpu.VMEM((8, G), f32), dma((2,))],
            compiler_params=pltpu.CompilerParams(vmem_limit_bytes=16 * 2**20),
            name="lay_more" if more else "lay",
        )(table, best, peaks, *tiles_and_blank)

    def few(mine, table, best, peaks, out, blank):
        return lay(False, table, best, peaks, out, pltpu.with_memory_space_constraint(blank, pltpu.HBM))

    def many(mine, table, best, peaks, out, blank):
        rest = share(mine, table)
        return lay(True, table, best, peaks, out, rest, pltpu.with_memory_space_constraint(blank, pltpu.HBM))

    blank = pltpu.with_memory_space_constraint(blank, pltpu.HBM)
    clones, peak, total = lax.switch(kind.reshape(()), [few, many], mine, table, best, peaks, out, blank)
    return (peak, clones, total.reshape(()))


def solution(mesh):
    return jax.shard_map(
        body,
        mesh=mesh,
        in_specs=(
            P(None, "gauss"),
            P(None, "gauss"),
            P(None, "gauss"),
            P(None, "gauss"),
            P("view", None, "gauss"),
            P("view", "gauss"),
            P("gauss"),
            P("view", None, None),
            P("view", None),
            P("view"),
        ),
        out_specs=(P(None, "gauss"), P(None, "gauss"), P()),
        check_vma=False,
    )
```

```python
import functools

import jax
import jax.numpy as jnp
from jax import lax
from jax.experimental import pallas as pl
from jax.experimental.pallas import tpu as pltpu
from jax.sharding import PartitionSpec as P

G = 16384
ROWS = 61
BLK = 128
CAP = G // BLK
NV = 8
NG = 32
PER = CAP // NG
CHUNKS = 4
FIRST = 60
MESH = pl.DeviceIdType.MESH
VMEM = pl.BlockSpec(memory_space=pltpu.VMEM)
SMEM = pl.BlockSpec(memory_space=pltpu.SMEM)
HBM = pl.BlockSpec(memory_space=pltpu.HBM)


def each(lo, n, do):
    if isinstance(lo, int) and isinstance(n, int):
        for i in range(lo, n):
            do(i)
        return

    def one(i, _):
        do(i)
        return 0

    lax.fori_loop(lo, n, one, 0)


def front_kernel(
    mask_h, means_h, scales_h, quats_h, grad_h, seen_h, rot_h, trans_h, focal_h, attrs,
    part, packed, tiles, count, blank,
    mask, means, scales, quats, grad, seen, rot, trans, focal,
    xa, xb, x, gl, picks, tab, stab, zeros, sem, load_sem, blank_sem,
):
    v = lax.axis_index("view")
    pairs = (
        (mask_h, mask), (rot_h, rot), (trans_h, trans), (focal_h, focal), (means_h, means), (scales_h, scales),
        (quats_h, quats), (seen_h, seen), (grad_h, grad),
    )
    loads = [pltpu.make_async_copy(src, dst, load_sem.at[i]) for i, (src, dst) in enumerate(pairs)]
    for load in loads:
        load.start()
    a_at = pl.multiple_of(jnp.clip(v - 2, 0, 5) * 8, 8)
    b_at = pl.multiple_of(jnp.clip(v - 1, 0, 5) * 8, 8)
    load_a = pltpu.make_async_copy(attrs.at[pl.ds(a_at, 8), :], xa, sem.at[0])
    load_b = pltpu.make_async_copy(attrs.at[pl.ds(b_at, 8), :], xb, sem.at[1])
    load_c = pltpu.make_async_copy(attrs.at[48:49, :], xb.at[0:1, :], sem.at[1])
    load_a.start()

    @pl.when(v < 7)
    def _():
        load_b.start()

    @pl.when(v == 7)
    def _():
        load_c.start()

    zeros[...] = jnp.zeros_like(zeros)
    fills = []
    for r in range(NV):
        lo, hi = 8 * r, min(8 * r + 8, ROWS)
        fills.append(pltpu.make_async_copy(zeros.at[0 : hi - lo, :], blank.at[lo:hi, :], blank_sem.at[r]))
    loads[0].wait()

    sub = lax.broadcasted_iota(jnp.int32, (8, 128), 0)
    lane = lax.broadcasted_iota(jnp.int32, (8, 128), 1)
    marks = mask[...].astype(jnp.float32).astype(jnp.bfloat16)
    i0 = lax.broadcasted_iota(jnp.int32, (128, 128), 0)
    i1 = lax.broadcasted_iota(jnp.int32, (128, 128), 1)
    upto = (i0 <= i1).astype(jnp.float32).astype(jnp.bfloat16)
    before = (i0 < i1).astype(jnp.float32).astype(jnp.bfloat16)
    after = (i0 > i1).astype(jnp.float32).astype(jnp.bfloat16)
    run = jnp.dot(marks, upto, preferred_element_type=jnp.float32).astype(jnp.int32)
    in_lanes = lax.dot_general(
        jnp.ones((8, 128), jnp.bfloat16), marks, (((1,), (1,)), ((), ())), preferred_element_type=jnp.float32
    )
    base = jnp.dot(in_lanes.astype(jnp.bfloat16), before, preferred_element_type=jnp.float32)
    end = base + in_lanes
    tab[...] = jnp.where(sub == 0, base, end).astype(jnp.int32)
    to_smem = pltpu.make_async_copy(tab, stab, sem.at[2])
    to_smem.start()
    total = jnp.sum(in_lanes, axis=1, keepdims=True)
    count[...] = jnp.broadcast_to(total, (8, 128)).astype(jnp.int32)

    in_row = jnp.dot(marks, jnp.ones((128, 128), jnp.bfloat16), preferred_element_type=jnp.float32)
    row_base = jnp.dot(after, in_row.astype(jnp.bfloat16), preferred_element_type=jnp.float32).astype(jnp.int32)
    e = jnp.where(mask[...] > 0, i1 + 128 + ((i1 - run + 1) << 8), 0)
    for bit in range(7):
        far = pltpu.roll(e, 128 - (1 << bit), axis=1)
        comes = (far & (256 << bit)) != 0
        goes = (e & (256 << bit)) != 0
        e = jnp.where(comes, far, jnp.where(goes, 0, e))
    e = e & 255
    turn = row_base & 127
    for bit in range(7):
        e = jnp.where((turn & (1 << bit)) != 0, pltpu.roll(e, 1 << bit, axis=1), e)
    picks[...] = e | jnp.where(i1 < turn, 256, 0)

    for load in loads[1:]:
        load.wait()
    for fill in fills:
        fill.start()

    def step(c, _):
        s = pl.ds(pl.multiple_of(c * 1024, 1024), 1024)

        def row(ref, *at):
            return ref[at[:-1] + (slice(at[-1], at[-1] + 1), s)].reshape(8, 128)

        m = [row(means, i) for i in range(3)]
        sc = [row(scales, i) for i in range(3)]
        q = [row(quats, i) for i in range(4)]
        inv = 1.0 / jnp.sqrt(q[0] * q[0] + q[1] * q[1] + q[2] * q[2] + q[3] * q[3] + 0.25)
        w, xq, y, z = (t * inv for t in q)
        rq = [
            [1 - 2 * (y * y + z * z), 2 * (xq * y - w * z), 2 * (xq * z + w * y)],
            [2 * (xq * y + w * z), 1 - 2 * (xq * xq + z * z), 2 * (y * z - w * xq)],
            [2 * (xq * z - w * y), 2 * (y * z + w * xq), 1 - 2 * (xq * xq + y * y)],
        ]
        factor = [[rq[i][j] * sc[j] for j in range(3)] for i in range(3)]
        gbest = jnp.zeros((8, 128), jnp.float32)
        lbest = jnp.zeros((8, 128), jnp.float32)
        for n in range(seen.shape[0]):
            r = [[rot[i, n, j] for j in range(3)] for i in range(3)]
            p = [r[i][0] * m[0] + r[i][1] * m[1] + r[i][2] * m[2] + trans[n, i] for i in range(3)]
            near = 1.0 / jnp.maximum(p[2], 1.0)
            j00 = focal[n] * near
            j02 = -j00 * p[0] * near
            j12 = -j00 * p[1] * near
            first = [j00 * r[0][j] + j02 * r[2][j] for j in range(3)]
            second = [j00 * r[1][j] + j12 * r[2][j] for j in range(3)]
            pr = [sum(first[j] * factor[j][k] for j in range(3)) for k in range(3)]
            qr = [sum(second[j] * factor[j][k] for j in range(3)) for k in range(3)]
            a = pr[0] * pr[0] + pr[1] * pr[1] + pr[2] * pr[2] + 0.3
            cc = qr[0] * qr[0] + qr[1] * qr[1] + qr[2] * qr[2] + 0.3
            b = pr[0] * qr[0] + pr[1] * qr[1] + pr[2] * qr[2]
            half = 0.5 * (a - cc)
            lam = 0.5 * (a + cc) + jnp.sqrt(half * half + b * b + 0.01)
            on = row(seen, n) > 0
            g0, g1 = row(grad, n, 0), row(grad, n, 1)
            gbest = jnp.maximum(gbest, jnp.where(on, g0 * g0 + g1 * g1, 0.0))
            lbest = jnp.maximum(lbest, jnp.where(on, lam, 0.0))
        piece, at = c // 2, pl.multiple_of((c % 2) * 8, 8)
        part[piece, 0, pl.ds(at, 8), :] = gbest
        part[piece, 1, pl.ds(at, 8), :] = lbest
        gl[0:1, s] = gbest.reshape(1, 1024)
        gl[1:2, s] = lbest.reshape(1, 1024)
        return 0

    lax.fori_loop(0, 16, step, 0, unroll=4)

    load_a.wait()

    @pl.when(v < 7)
    def _():
        load_b.wait()

    @pl.when(v == 7)
    def _():
        load_c.wait()

    @pl.when(v == 0)
    def _():
        x[0:3, :] = means[...]
        x[3:6, :] = scales[...]
        x[6:8, :] = quats[0:2, :]

    @pl.when(v == 1)
    def _():
        x[0:2, :] = quats[2:4, :]
        x[2:8, :] = xb[0:6, :]

    @pl.when((v > 1) & (v < 7))
    def _():
        x[0:2, :] = xa[6:8, :]
        x[2:8, :] = xb[0:6, :]

    @pl.when(v == 7)
    def _():
        x[0:2, :] = xa[6:8, :]
        x[2:3, :] = xb[0:1, :]
        x[3:8, :] = jnp.zeros((5, G), jnp.float32)

    to_smem.wait()

    def pack(c, carry):
        block = stab[0, c] >> 7
        full = (stab[1, c] >> 7) > block
        cols = pl.ds(pl.multiple_of(c * 128, 128), 128)
        pick = jnp.broadcast_to(picks[pl.ds(c, 1), :], (8, 128))
        at, kind = pick & 127, pick & 384
        here, later = kind == 128, kind == 384
        done = []
        for ref, old in zip((x, gl), carry):
            got = jnp.take_along_axis(ref[:, cols], at, axis=1, mode="promise_in_bounds")
            now = jnp.where(here, got, old)
            done.append((now, jnp.where(full, jnp.where(later, got, 0.0), now)))
        tiles[block] = done[0][0]
        packed[block] = done[1][0][0:2]
        return done[0][1], done[1][1]

    zero = jnp.zeros((8, 128), jnp.float32)
    left = lax.fori_loop(0, 128, pack, (zero, zero), unroll=32)
    last = stab[1, 127]

    @pl.when(last < G)
    def _():
        tiles[last >> 7] = left[0]
        packed[last >> 7] = left[1][0:2]

    for fill in fills:
        fill.wait()


def spread(out, size, source, mine, s_own, r_own, s_side, r_side, s_far, r_far, ready):
    v = lax.axis_index("view")
    core, chip = v % 2, v // 2
    mate = chip * 2 + 1 - core
    right, left, far = (((chip + i) % 4) * 2 + core for i in (1, 3, 2))
    rows = pl.ds(pl.multiple_of(v * 8, 8), 8)

    def place(q, _):
        out[rows, pl.ds(pl.multiple_of(q * BLK, BLK), BLK)] = mine[source(q)]
        return 0

    lax.fori_loop(0, size, place, 0, unroll=4)
    ready()
    wide = size * BLK // CHUNKS

    def over_view(peer, group, c, s, r):
        at = out.at[pl.ds(pl.multiple_of(group * 8, 8), 8), c * wide : (c + 1) * wide]
        return pltpu.make_async_remote_copy(at, at, s, r, device_id={"view": peer}, device_id_type=MESH)

    def side(kind, c, group):
        return over_view(mate, group, c, s_side.at[kind, c], r_side.at[kind, c])

    def go(way, c, group):
        return over_view(right if way == 0 else left, group, c, s_own.at[way, c], r_own.at[way, c])

    def on(way, c, group):
        return over_view(right if way == 0 else left, group, c, s_far.at[c], r_far.at[c])

    for c in range(CHUNKS):
        go(0, c, v).start()
        go(1, c, v).start()
        side(0, c, v).start()
    for c in range(CHUNKS):
        go(0, c, left).wait_recv()
        if c < CHUNKS // 2:
            on(0, c, left).start()
        side(2, c, left).start()
        go(1, c, right).wait_recv()
        if c >= CHUNKS // 2:
            on(1, c, right).start()
        side(1, c, right).start()
    for c in range(CHUNKS):
        on(0, c, far).wait_recv()
        side(3, c, far).start()
    across = [mate, right + 1 - 2 * core, left + 1 - 2 * core, far + 1 - 2 * core]
    for c in range(CHUNKS):
        for kind in range(4):
            side(kind, c, across[kind]).wait_recv()
            side(kind, c, v).wait_send()
        go(0, c, v).wait_send()
        go(1, c, v).wait_send()
        on(0, c, v).wait_send()


def move_kernel(
    part, packed, tiles, count,
    mine, out, peaks, best, counts, table, kind,
    taken, takenp, merged, mergedp, top, turned, turnedp, tab, stab,
    s_part, r_part, s_pack, r_pack, s_best, r_best, s_peak, r_peak, s_count, r_count, s_pair, r_pair, s_top, r_top,
    s_own, r_own, s_side, r_side, s_far, r_far, own,
):
    v, g = lax.axis_index("view"), lax.axis_index("gauss")
    gy, gz = g // 8, g % 8
    barrier = pltpu.get_barrier_semaphore()
    each(1, NV, lambda i: pl.semaphore_signal(barrier, inc=1, device_id={"view": (v + i) % NV}, device_id_type=MESH))
    each(1, NG, lambda i: pl.semaphore_signal(barrier, inc=1, device_id={"gauss": (g + i) % NG}, device_id_type=MESH))
    pl.semaphore_wait(barrier, NV - 1 + NG - 1)

    def over_view(peer, src, dst, s, r):
        return pltpu.make_async_remote_copy(src, dst, s, r, device_id={"view": peer}, device_id_type=MESH)

    def over_gauss(peer, src, dst, s, r):
        return pltpu.make_async_remote_copy(src, dst, s, r, device_id={"gauss": peer}, device_id_type=MESH)

    def owner(i):
        return ((gy + i // 8) % 4) * 8 + (gz + i % 8) % 8

    def tell(i, slot):
        return over_gauss((g + i) % NG, count, counts.at[slot], s_count.at[i], r_count.at[slot])

    def give_part(i, slot):
        peer = (v + i) % NV
        return over_view(peer, part.at[peer], taken.at[slot], s_part.at[i], r_part.at[slot])

    def give_best(i, slot):
        return over_view((v + i) % NV, merged, best.at[slot], s_best.at[i], r_best.at[slot])

    def give_pack(i, slot):
        peer = (v + i) % NV
        return over_view(peer, turnedp.at[pl.ds(peer * 16, 16)], takenp.at[slot], s_pack.at[i], r_pack.at[slot])

    def give_top(t):
        at = pl.ds(t * PER, PER)
        return over_gauss(owner(v * 4 + t), mergedp.at[at], top.at[at], s_top.at[t], r_top.at[t])

    each(1, NG, lambda i: tell(i, g).start())
    each(1, NV, lambda i: give_part(i, v).start())
    counts[g] = count[...]
    each(1, NG, lambda i: tell(i, (g + i) % NG).wait_recv())

    def add(s, mine):
        return mine + jnp.where(s < g, (counts[s] + (BLK - 1)) >> 7, 0)

    tab[...] = lax.fori_loop(0, NG, add, jnp.zeros((8, 128), jnp.int32))
    to_smem = pltpu.make_async_copy(tab, stab, own.at[0])
    to_smem.start()
    to_smem.wait()
    shift = stab[0, 0]

    def pair(i):
        at = pl.ds(i * PER, PER)
        return over_gauss(owner(i), turned.at[at], mine.at[at], s_pair.at[i], r_pair.at[i])

    keep = pltpu.make_async_copy(turned.at[0:PER], mine.at[0:PER], own.at[1])

    def turn(i):
        block = (owner(i) - shift) & (NG - 1)
        for w in range(PER):
            turned[i * PER + w] = tiles[block + w * NG]
            turnedp[i * PER + w] = packed[block + w * NG]

    for i in range(NG + 2):
        if i < NG:
            turn(i)
        if i > 2:
            pair(i - 2).start()
    keep.start()
    each(1, NV, lambda i: give_pack(i, v).start())

    def first():
        each(1, NV, lambda i: give_part(i, (v + i) % NV).wait_recv())
        so_far = lax.fori_loop(1, NV, lambda i, so: jnp.maximum(so, taken[(v + i) % NV]), part[v])
        merged[...] = so_far
        best[v] = so_far
        each(1, NV, lambda i: give_best(i, v).start())

    def second():
        each(1, NV, lambda i: give_pack(i, (v + i) % NV).wait_recv())
        best_p = lax.fori_loop(1, NV, lambda i, so: jnp.maximum(so, takenp[(v + i) % NV]), turnedp[pl.ds(v * 16, 16)])
        mergedp[...] = best_p

        @pl.when(v > 0)
        def _():
            give_top(0).start()

        @pl.when(v == 0)
        def _():
            top[0:PER] = best_p[0:PER]

        each(1, 4, lambda t: give_top(t).start())

    def third():
        @pl.when(v > 0)
        def _():
            give_top(0).wait_recv()

        each(1, 4, lambda t: give_top(t).wait_recv())

    first()

    sub = lax.broadcasted_iota(jnp.int32, (8, 128), 0)
    k = lax.broadcasted_iota(jnp.int32, (8, 128), 1) * NG + g
    off = jnp.zeros((8, 128), jnp.int32)
    every = jnp.zeros((8, 128), jnp.int32)
    source = jnp.zeros((8, 128), jnp.int32)
    for s in range(NG):
        n = counts[s]
        blocks = (n + (BLK - 1)) >> 7
        where = (((gy - s // 8) & 3) * 8 + ((gz - s % 8) & 7)) * PER
        inside = (k >= off) & (k < off + blocks)
        source = jnp.where(inside, where + ((k - off) >> 5), source)
        off = off + blocks
        every = every + n
    slots = (off - g + (NG - 1)) >> 5
    most = (off + (NG - 1)) >> 5
    more = (most > FIRST).astype(jnp.int32)
    filled = jnp.where(sub == 0, source, jnp.where(sub == 1, every, jnp.where(sub == 2, slots, more)))
    table[...] = filled
    tab[...] = filled
    pick_smem = pltpu.make_async_copy(tab, stab, own.at[0])
    pick_smem.start()

    second()
    third()
    pick_smem.wait()
    kind[0, 0] = stab[3, 0]

    def give_peak(i, slot):
        at = peaks.at[pl.ds(slot * 16, 16)]
        return over_view((v + i) % NV, top, at, s_peak.at[i], r_peak.at[slot])

    each(1, NV, lambda i: give_peak(i, v).start())
    peaks[pl.ds(v * 16, 16)] = top[...]
    keep.wait()
    each(1, NG, lambda i: pair(i).wait_recv())
    spread(
        out, FIRST, lambda q: stab[0, q], mine, s_own, r_own, s_side, r_side, s_far, r_far, lambda: None
    )
    each(1, NV, lambda i: give_peak(i, (v + i) % NV).wait_recv())
    each(1, NV, lambda i: give_peak(i, v).wait_send())
    each(1, NV, lambda i: give_best(i, (v + i) % NV).wait_recv())

    each(1, NG, lambda i: tell(i, g).wait_send())
    each(1, NG, lambda i: pair(i).wait_send())
    each(1, NV, lambda i: give_part(i, v).wait_send())
    each(1, NV, lambda i: give_pack(i, v).wait_send())
    each(1, NV, lambda i: give_best(i, v).wait_send())

    @pl.when(v > 0)
    def _():
        give_top(0).wait_send()

    each(1, 4, lambda t: give_top(t).wait_send())


def share_kernel(mine, table, out, *sems):
    v = lax.axis_index("view")
    barrier = pltpu.get_barrier_semaphore()
    each(1, NV, lambda i: pl.semaphore_signal(barrier, inc=1, device_id={"view": (v + i) % NV}, device_id_type=MESH))
    spread(out, CAP - FIRST, lambda q: table[0, FIRST + q], mine, *sems, lambda: pl.semaphore_wait(barrier, NV - 1))


def lay_kernel(more, table, best, peaks, tiles, *refs):
    rest, _, clones, peak, total, stage, sem = refs if more else (None, *refs)
    sub = lax.broadcasted_iota(jnp.int32, (8, 128), 0)
    used = table[2, 0]
    total[0, 0] = table[1, 0]

    def cols(at):
        return pl.ds(pl.multiple_of(at * BLK, BLK), BLK)

    def runs(count, most):
        for n in (64, 32, 16, 8, 4, 2, 1):
            if n <= most:
                yield (count & n) != 0, pl.multiple_of((count & (256 - 2 * n)) * BLK, BLK), n * BLK

    if more:
        pieces = [(tiles, 0, (True, 0, FIRST * BLK))]
        pieces += [(rest, FIRST, run) for run in runs(used - FIRST, CAP - FIRST)]
    else:
        pieces = [(tiles, 0, run) for run in runs(used, FIRST)]
    main, last = [], []
    for src, first, (on, at, size) in pieces:
        to = pl.multiple_of(at + first * BLK, BLK)
        main.append((on, pltpu.make_async_copy(
            src.at[0:56, pl.ds(at, size)], clones.at[0:56, pl.ds(to, size)], sem.at[0]
        )))
        last.append((on, pltpu.make_async_copy(
            stage.at[0 : ROWS - 56, pl.ds(to, size)], clones.at[56:ROWS, pl.ds(to, size)], sem.at[1]
        )))
    for on, copy in main:
        pl.when(on)(copy.start)

    def finish(src, first):
        def one(q):
            tops = peaks[table[0, q]]
            gtop = jnp.broadcast_to(jnp.sqrt(tops[0:1]), (8, 128))
            ltop = jnp.broadcast_to(3.0 * jnp.sqrt(tops[1:2]), (8, 128))
            tile = src[56:64, cols(q - first)]
            stage[:, cols(q)] = jnp.where(sub == 3, gtop, jnp.where(sub == 4, ltop, tile))

        return one

    each(jnp.int32(0), jnp.minimum(used, FIRST), finish(tiles, 0))
    if more:
        each(jnp.int32(FIRST), used, finish(rest, FIRST))
    for on, copy in last:
        pl.when(on)(copy.start)

    def roots(c, _):
        s = pl.ds(pl.multiple_of(c * 1024, 1024), 1024)
        piece, at = c // 2, pl.multiple_of((c % 2) * 8, 8)
        peak[0:1, s] = jnp.sqrt(best[piece, 0, pl.ds(at, 8), :]).reshape(1, 1024)
        peak[1:2, s] = (3.0 * jnp.sqrt(best[piece, 1, pl.ds(at, 8), :])).reshape(1, 1024)
        return 0

    lax.fori_loop(0, 16, roots, 0)
    for on, copy in main + last:
        pl.when(on)(copy.wait)


def body(means, scales, quats, attrs, grad_screen, visible, clone_mask, rotation, shift, focal):
    f32, i32 = jnp.float32, jnp.int32
    shape = jax.ShapeDtypeStruct
    dma = pltpu.SemaphoreType.DMA
    view_sems = [dma((2, CHUNKS))] * 2 + [dma((4, CHUNKS))] * 2 + [dma((CHUNKS,))] * 2
    mask = clone_mask.reshape(128, 128)
    part, packed, tiles, count, blank = pl.pallas_call(
        front_kernel,
        in_specs=[HBM] * 10,
        out_specs=(VMEM,) * 4 + (HBM,),
        out_shape=(
            shape((NV, 2, 16, 128), f32),
            shape((CAP, 2, 128), f32),
            shape((CAP, 8, 128), f32),
            shape((8, 128), i32),
            shape((ROWS, G), f32),
        ),
        scratch_shapes=[
            pltpu.VMEM((128, 128), i32),
            pltpu.VMEM((3, G), f32),
            pltpu.VMEM((3, G), f32),
            pltpu.VMEM((4, G), f32),
            pltpu.VMEM((4, 2, G), f32),
            pltpu.VMEM((4, G), i32),
            pltpu.SMEM((3, 4, 3), f32),
            pltpu.SMEM((4, 3), f32),
            pltpu.SMEM((4,), f32),
            pltpu.VMEM((8, G), f32),
            pltpu.VMEM((8, G), f32),
            pltpu.VMEM((8, G), f32),
            pltpu.VMEM((8, G), f32),
            pltpu.VMEM((128, 128), i32),
            pltpu.VMEM((8, 128), i32),
            pltpu.SMEM((8, 128), i32),
            pltpu.VMEM((8, G), f32),
            dma((3,)),
            dma((9,)),
            dma((NV,)),
        ],
        compiler_params=pltpu.CompilerParams(vmem_limit_bytes=16 * 2**20),
        name="front",
    )(
        *(
            pltpu.with_memory_space_constraint(a, pltpu.HBM)
            for a in (mask, means, scales, quats, grad_screen, visible, rotation.transpose(1, 0, 2), shift, focal, attrs)
        )
    )

    mine, out, peaks, best, _, table, kind = pl.pallas_call(
        move_kernel,
        in_specs=[VMEM] * 4,
        out_specs=(VMEM,) * 6 + (SMEM,),
        out_shape=(
            shape((CAP, 8, 128), f32),
            shape((8 * NV, FIRST * BLK), f32),
            shape((CAP, 2, 128), f32),
            shape((NV, 2, 16, 128), f32),
            shape((NG, 8, 128), i32),
            shape((8, 128), i32),
            shape((1, 1), i32),
        ),
        scratch_shapes=[
            pltpu.VMEM((NV, 2, 16, 128), f32),
            pltpu.VMEM((NV, 16, 2, 128), f32),
            pltpu.VMEM((2, 16, 128), f32),
            pltpu.VMEM((16, 2, 128), f32),
            pltpu.VMEM((16, 2, 128), f32),
            pltpu.VMEM((CAP, 8, 128), f32),
            pltpu.VMEM((CAP, 2, 128), f32),
            pltpu.VMEM((8, 128), i32),
            pltpu.SMEM((8, 128), i32),
        ]
        + [dma((NV,))] * 8
        + [dma((NG,))] * 4
        + [dma((4,))] * 2
        + view_sems
        + [dma((2,))],
        compiler_params=pltpu.CompilerParams(
            collective_id=0, has_side_effects=True, vmem_limit_bytes=16 * 2**20
        ),
        name="move",
    )(part, packed, tiles, count)

    share = pl.pallas_call(
        share_kernel,
        in_specs=[VMEM, SMEM],
        out_specs=VMEM,
        out_shape=shape((8 * NV, (CAP - FIRST) * BLK), f32),
        scratch_shapes=view_sems,
        compiler_params=pltpu.CompilerParams(
            collective_id=1, has_side_effects=True, vmem_limit_bytes=16 * 2**20
        ),
        name="share",
    )

    def lay(more, table, best, peaks, *tiles_and_blank):
        return pl.pallas_call(
            functools.partial(lay_kernel, more),
            in_specs=[SMEM, VMEM, VMEM] + [VMEM] * (1 + more) + [HBM],
            out_specs=(HBM, VMEM, SMEM),
            out_shape=(shape((ROWS, G), f32), shape((2, G), f32), shape((1, 1), i32)),
            input_output_aliases={4 + more: 0},
            scratch_shapes=[pltpu.VMEM((8, G), f32), dma((2,))],
            compiler_params=pltpu.CompilerParams(vmem_limit_bytes=16 * 2**20),
            name="lay_more" if more else "lay",
        )(table, best, peaks, *tiles_and_blank)

    def few(mine, table, best, peaks, out, blank):
        return lay(False, table, best, peaks, out, pltpu.with_memory_space_constraint(blank, pltpu.HBM))

    def many(mine, table, best, peaks, out, blank):
        rest = share(mine, table)
        return lay(True, table, best, peaks, out, rest, pltpu.with_memory_space_constraint(blank, pltpu.HBM))

    blank = pltpu.with_memory_space_constraint(blank, pltpu.HBM)
    clones, peak, total = lax.switch(kind.reshape(()), [few, many], mine, table, best, peaks, out, blank)
    return (peak, clones, total.reshape(()))


def solution(mesh):
    return jax.shard_map(
        body,
        mesh=mesh,
        in_specs=(
            P(None, "gauss"),
            P(None, "gauss"),
            P(None, "gauss"),
            P(None, "gauss"),
            P("view", None, "gauss"),
            P("view", "gauss"),
            P("gauss"),
            P("view", None, None),
            P("view", None),
            P("view"),
        ),
        out_specs=(P(None, "gauss"), P(None, "gauss"), P()),
        check_vma=False,
    )
```

```python
import functools

import jax
import jax.numpy as jnp
from jax import lax
from jax.experimental import pallas as pl
from jax.experimental.pallas import tpu as pltpu
from jax.sharding import PartitionSpec as P

G = 16384
ROWS = 61
BLK = 128
CAP = G // BLK
NV = 8
NG = 32
PER = CAP // NG
CHUNKS = 4
FIRST = 60
MESH = pl.DeviceIdType.MESH
VMEM = pl.BlockSpec(memory_space=pltpu.VMEM)
SMEM = pl.BlockSpec(memory_space=pltpu.SMEM)
HBM = pl.BlockSpec(memory_space=pltpu.HBM)


def each(lo, n, do):
    if isinstance(lo, int) and isinstance(n, int):
        for i in range(lo, n):
            do(i)
        return

    def one(i, _):
        do(i)
        return 0

    lax.fori_loop(lo, n, one, 0)


def front_kernel(
    mask_h, means_h, scales_h, quats_h, grad_h, seen_h, rot_h, trans_h, focal_h, attrs,
    part, packed, tiles, count, blank,
    mask, means, scales, quats, grad, seen, rot, trans, focal,
    xa, xb, x, gl, picks, tab, stab, zeros, sem, load_sem, blank_sem,
):
    v = lax.axis_index("view")
    pairs = (
        (mask_h, mask), (rot_h, rot), (trans_h, trans), (focal_h, focal), (means_h, means), (scales_h, scales),
        (quats_h, quats), (seen_h, seen), (grad_h, grad),
    )
    loads = [pltpu.make_async_copy(src, dst, load_sem.at[i]) for i, (src, dst) in enumerate(pairs)]
    for load in loads:
        load.start()
    a_at = pl.multiple_of(jnp.clip(v - 2, 0, 5) * 8, 8)
    b_at = pl.multiple_of(jnp.clip(v - 1, 0, 5) * 8, 8)
    load_a = pltpu.make_async_copy(attrs.at[pl.ds(a_at, 8), :], xa, sem.at[0])
    load_b = pltpu.make_async_copy(attrs.at[pl.ds(b_at, 8), :], xb, sem.at[1])
    load_c = pltpu.make_async_copy(attrs.at[48:49, :], xb.at[0:1, :], sem.at[1])
    load_a.start()

    @pl.when(v < 7)
    def _():
        load_b.start()

    @pl.when(v == 7)
    def _():
        load_c.start()

    zeros[...] = jnp.zeros_like(zeros)
    fills = []
    for r in range(NV):
        lo, hi = 8 * r, min(8 * r + 8, ROWS)
        fills.append(pltpu.make_async_copy(zeros.at[0 : hi - lo, :], blank.at[lo:hi, :], blank_sem.at[r]))
    loads[0].wait()

    sub = lax.broadcasted_iota(jnp.int32, (8, 128), 0)
    lane = lax.broadcasted_iota(jnp.int32, (8, 128), 1)
    marks = mask[...].astype(jnp.float32).astype(jnp.bfloat16)
    i0 = lax.broadcasted_iota(jnp.int32, (128, 128), 0)
    i1 = lax.broadcasted_iota(jnp.int32, (128, 128), 1)
    upto = (i0 <= i1).astype(jnp.float32).astype(jnp.bfloat16)
    before = (i0 < i1).astype(jnp.float32).astype(jnp.bfloat16)
    after = (i0 > i1).astype(jnp.float32).astype(jnp.bfloat16)
    run = jnp.dot(marks, upto, preferred_element_type=jnp.float32).astype(jnp.int32)
    in_lanes = lax.dot_general(
        jnp.ones((8, 128), jnp.bfloat16), marks, (((1,), (1,)), ((), ())), preferred_element_type=jnp.float32
    )
    base = jnp.dot(in_lanes.astype(jnp.bfloat16), before, preferred_element_type=jnp.float32)
    end = base + in_lanes
    tab[...] = jnp.where(sub == 0, base, end).astype(jnp.int32)
    to_smem = pltpu.make_async_copy(tab, stab, sem.at[2])
    to_smem.start()
    total = jnp.sum(in_lanes, axis=1, keepdims=True)
    count[...] = jnp.broadcast_to(total, (8, 128)).astype(jnp.int32)

    in_row = jnp.dot(marks, jnp.ones((128, 128), jnp.bfloat16), preferred_element_type=jnp.float32)
    row_base = jnp.dot(after, in_row.astype(jnp.bfloat16), preferred_element_type=jnp.float32).astype(jnp.int32)
    e = jnp.where(mask[...] > 0, i1 + 128 + ((i1 - run + 1) << 8), 0)
    for bit in range(7):
        far = pltpu.roll(e, 128 - (1 << bit), axis=1)
        comes = (far & (256 << bit)) != 0
        goes = (e & (256 << bit)) != 0
        e = jnp.where(comes, far, jnp.where(goes, 0, e))
    e = e & 255
    turn = row_base & 127
    for bit in range(7):
        e = jnp.where((turn & (1 << bit)) != 0, pltpu.roll(e, 1 << bit, axis=1), e)
    picks[...] = e | jnp.where(i1 < turn, 256, 0)

    for load in loads[1:]:
        load.wait()
    for fill in fills:
        fill.start()

    def step(c, _):
        s = pl.ds(pl.multiple_of(c * 1024, 1024), 1024)

        def row(ref, *at):
            return ref[at[:-1] + (slice(at[-1], at[-1] + 1), s)].reshape(8, 128)

        m = [row(means, i) for i in range(3)]
        sc = [row(scales, i) for i in range(3)]
        q = [row(quats, i) for i in range(4)]
        inv = 1.0 / jnp.sqrt(q[0] * q[0] + q[1] * q[1] + q[2] * q[2] + q[3] * q[3] + 0.25)
        w, xq, y, z = (t * inv for t in q)
        rq = [
            [1 - 2 * (y * y + z * z), 2 * (xq * y - w * z), 2 * (xq * z + w * y)],
            [2 * (xq * y + w * z), 1 - 2 * (xq * xq + z * z), 2 * (y * z - w * xq)],
            [2 * (xq * z - w * y), 2 * (y * z + w * xq), 1 - 2 * (xq * xq + y * y)],
        ]
        factor = [[rq[i][j] * sc[j] for j in range(3)] for i in range(3)]
        gbest = jnp.zeros((8, 128), jnp.float32)
        lbest = jnp.zeros((8, 128), jnp.float32)
        for n in range(seen.shape[0]):
            r = [[rot[i, n, j] for j in range(3)] for i in range(3)]
            p = [r[i][0] * m[0] + r[i][1] * m[1] + r[i][2] * m[2] + trans[n, i] for i in range(3)]
            near = 1.0 / jnp.maximum(p[2], 1.0)
            j00 = focal[n] * near
            j02 = -j00 * p[0] * near
            j12 = -j00 * p[1] * near
            first = [j00 * r[0][j] + j02 * r[2][j] for j in range(3)]
            second = [j00 * r[1][j] + j12 * r[2][j] for j in range(3)]
            pr = [sum(first[j] * factor[j][k] for j in range(3)) for k in range(3)]
            qr = [sum(second[j] * factor[j][k] for j in range(3)) for k in range(3)]
            a = pr[0] * pr[0] + pr[1] * pr[1] + pr[2] * pr[2] + 0.3
            cc = qr[0] * qr[0] + qr[1] * qr[1] + qr[2] * qr[2] + 0.3
            b = pr[0] * qr[0] + pr[1] * qr[1] + pr[2] * qr[2]
            half = 0.5 * (a - cc)
            lam = 0.5 * (a + cc) + jnp.sqrt(half * half + b * b + 0.01)
            on = row(seen, n) > 0
            g0, g1 = row(grad, n, 0), row(grad, n, 1)
            gbest = jnp.maximum(gbest, jnp.where(on, g0 * g0 + g1 * g1, 0.0))
            lbest = jnp.maximum(lbest, jnp.where(on, lam, 0.0))
        piece, at = c // 2, pl.multiple_of((c % 2) * 8, 8)
        part[piece, 0, pl.ds(at, 8), :] = gbest
        part[piece, 1, pl.ds(at, 8), :] = lbest
        gl[0:1, s] = gbest.reshape(1, 1024)
        gl[1:2, s] = lbest.reshape(1, 1024)
        return 0

    lax.fori_loop(0, 16, step, 0, unroll=4)

    load_a.wait()

    @pl.when(v < 7)
    def _():
        load_b.wait()

    @pl.when(v == 7)
    def _():
        load_c.wait()

    @pl.when(v == 0)
    def _():
        x[0:3, :] = means[...]
        x[3:6, :] = scales[...]
        x[6:8, :] = quats[0:2, :]

    @pl.when(v == 1)
    def _():
        x[0:2, :] = quats[2:4, :]
        x[2:8, :] = xb[0:6, :]

    @pl.when((v > 1) & (v < 7))
    def _():
        x[0:2, :] = xa[6:8, :]
        x[2:8, :] = xb[0:6, :]

    @pl.when(v == 7)
    def _():
        x[0:2, :] = xa[6:8, :]
        x[2:3, :] = xb[0:1, :]
        x[3:8, :] = jnp.zeros((5, G), jnp.float32)

    to_smem.wait()

    def pack(c, carry):
        block = stab[0, c] >> 7
        full = (stab[1, c] >> 7) > block
        cols = pl.ds(pl.multiple_of(c * 128, 128), 128)
        pick = jnp.broadcast_to(picks[pl.ds(c, 1), :], (8, 128))
        at, kind = pick & 127, pick & 384
        here, later = kind == 128, kind == 384
        done = []
        for ref, old in zip((x, gl), carry):
            got = jnp.take_along_axis(ref[:, cols], at, axis=1, mode="promise_in_bounds")
            now = jnp.where(here, got, old)
            done.append((now, jnp.where(full, jnp.where(later, got, 0.0), now)))
        tiles[block] = done[0][0]
        packed[block] = done[1][0][0:2]
        return done[0][1], done[1][1]

    zero = jnp.zeros((8, 128), jnp.float32)
    left = lax.fori_loop(0, 128, pack, (zero, zero), unroll=32)
    last = stab[1, 127]

    @pl.when(last < G)
    def _():
        tiles[last >> 7] = left[0]
        packed[last >> 7] = left[1][0:2]

    for fill in fills:
        fill.wait()


def spread(out, size, source, mine, s_own, r_own, s_side, r_side, s_far, r_far, ready):
    v = lax.axis_index("view")
    core, chip = v % 2, v // 2
    mate = chip * 2 + 1 - core
    right, left, far = (((chip + i) % 4) * 2 + core for i in (1, 3, 2))
    rows = pl.ds(pl.multiple_of(v * 8, 8), 8)

    def place(q, _):
        out[rows, pl.ds(pl.multiple_of(q * BLK, BLK), BLK)] = mine[source(q)]
        return 0

    wide = size * BLK // CHUNKS

    def over_view(peer, group, c, s, r):
        at = out.at[pl.ds(pl.multiple_of(group * 8, 8), 8), c * wide : (c + 1) * wide]
        return pltpu.make_async_remote_copy(at, at, s, r, device_id={"view": peer}, device_id_type=MESH)

    def side(kind, c, group):
        return over_view(mate, group, c, s_side.at[kind, c], r_side.at[kind, c])

    def go(way, c, group):
        return over_view(right if way == 0 else left, group, c, s_own.at[way, c], r_own.at[way, c])

    def on(way, c, group):
        return over_view(right if way == 0 else left, group, c, s_far.at[c], r_far.at[c])

    per = size // CHUNKS
    for c in range(CHUNKS + 1):
        if c < CHUNKS:
            lax.fori_loop(c * per, (c + 1) * per, place, 0, unroll=True)
        if c == 0:
            ready()
        else:
            go(0, c - 1, v).start()
            go(1, c - 1, v).start()
            side(0, c - 1, v).start()
    for c in range(CHUNKS):
        go(0, c, left).wait_recv()
        if c < CHUNKS // 2:
            on(0, c, left).start()
        side(2, c, left).start()
        go(1, c, right).wait_recv()
        if c >= CHUNKS // 2:
            on(1, c, right).start()
        side(1, c, right).start()
    for c in range(CHUNKS):
        on(0, c, far).wait_recv()
        side(3, c, far).start()
    across = [mate, right + 1 - 2 * core, left + 1 - 2 * core, far + 1 - 2 * core]
    for c in range(CHUNKS):
        for kind in range(4):
            side(kind, c, across[kind]).wait_recv()
            side(kind, c, v).wait_send()
        go(0, c, v).wait_send()
        go(1, c, v).wait_send()
        on(0, c, v).wait_send()


def move_kernel(
    part, packed, tiles, count,
    mine, out, peaks, best, counts, table, kind,
    taken, takenp, merged, mergedp, top, turned, turnedp, tab, stab,
    s_part, r_part, s_pack, r_pack, s_best, r_best, s_peak, r_peak, s_count, r_count, s_pair, r_pair, s_top, r_top,
    s_own, r_own, s_side, r_side, s_far, r_far, own,
):
    v, g = lax.axis_index("view"), lax.axis_index("gauss")
    gy, gz = g // 8, g % 8
    barrier = pltpu.get_barrier_semaphore()
    each(1, NV, lambda i: pl.semaphore_signal(barrier, inc=1, device_id={"view": (v + i) % NV}, device_id_type=MESH))
    each(1, NG, lambda i: pl.semaphore_signal(barrier, inc=1, device_id={"gauss": (g + i) % NG}, device_id_type=MESH))
    pl.semaphore_wait(barrier, NV - 1 + NG - 1)

    def over_view(peer, src, dst, s, r):
        return pltpu.make_async_remote_copy(src, dst, s, r, device_id={"view": peer}, device_id_type=MESH)

    def over_gauss(peer, src, dst, s, r):
        return pltpu.make_async_remote_copy(src, dst, s, r, device_id={"gauss": peer}, device_id_type=MESH)

    def owner(i):
        return ((gy + i // 8) % 4) * 8 + (gz + i % 8) % 8

    def tell(i, slot):
        return over_gauss((g + i) % NG, count, counts.at[slot], s_count.at[i], r_count.at[slot])

    def give_part(i, slot):
        peer = (v + i) % NV
        return over_view(peer, part.at[peer], taken.at[slot], s_part.at[i], r_part.at[slot])

    def give_best(i, slot):
        return over_view((v + i) % NV, merged, best.at[slot], s_best.at[i], r_best.at[slot])

    def give_pack(i, slot):
        peer = (v + i) % NV
        return over_view(peer, turnedp.at[pl.ds(peer * 16, 16)], takenp.at[slot], s_pack.at[i], r_pack.at[slot])

    def give_top(t):
        at = pl.ds(t * PER, PER)
        return over_gauss(owner(v * 4 + t), mergedp.at[at], top.at[at], s_top.at[t], r_top.at[t])

    each(1, NG, lambda i: tell(i, g).start())
    each(1, NV, lambda i: give_part(i, v).start())
    counts[g] = count[...]
    each(1, NG, lambda i: tell(i, (g + i) % NG).wait_recv())

    def add(s, mine):
        return mine + jnp.where(s < g, (counts[s] + (BLK - 1)) >> 7, 0)

    tab[...] = lax.fori_loop(0, NG, add, jnp.zeros((8, 128), jnp.int32))
    to_smem = pltpu.make_async_copy(tab, stab, own.at[0])
    to_smem.start()
    to_smem.wait()
    shift = stab[0, 0]

    def pair(i):
        at = pl.ds(i * PER, PER)
        return over_gauss(owner(i), turned.at[at], mine.at[at], s_pair.at[i], r_pair.at[i])

    keep = pltpu.make_async_copy(turned.at[0:PER], mine.at[0:PER], own.at[1])

    def turn(i):
        block = (owner(i) - shift) & (NG - 1)
        for w in range(PER):
            turned[i * PER + w] = tiles[block + w * NG]
            turnedp[i * PER + w] = packed[block + w * NG]

    for i in range(NG + 2):
        if i < NG:
            turn(i)
        if i > 2:
            pair(i - 2).start()
    keep.start()
    each(1, NV, lambda i: give_pack(i, v).start())

    def first():
        each(1, NV, lambda i: give_part(i, (v + i) % NV).wait_recv())
        so_far = lax.fori_loop(1, NV, lambda i, so: jnp.maximum(so, taken[(v + i) % NV]), part[v])
        merged[...] = so_far
        best[v] = so_far
        each(1, NV, lambda i: give_best(i, v).start())

    def second():
        each(1, NV, lambda i: give_pack(i, (v + i) % NV).wait_recv())
        best_p = lax.fori_loop(1, NV, lambda i, so: jnp.maximum(so, takenp[(v + i) % NV]), turnedp[pl.ds(v * 16, 16)])
        mergedp[...] = best_p

        @pl.when(v > 0)
        def _():
            give_top(0).start()

        @pl.when(v == 0)
        def _():
            top[0:PER] = best_p[0:PER]

        each(1, 4, lambda t: give_top(t).start())

    def third():
        @pl.when(v > 0)
        def _():
            give_top(0).wait_recv()

        each(1, 4, lambda t: give_top(t).wait_recv())

    first()

    sub = lax.broadcasted_iota(jnp.int32, (8, 128), 0)
    k = lax.broadcasted_iota(jnp.int32, (8, 128), 1) * NG + g
    off = jnp.zeros((8, 128), jnp.int32)
    every = jnp.zeros((8, 128), jnp.int32)
    source = jnp.zeros((8, 128), jnp.int32)
    for s in range(NG):
        n = counts[s]
        blocks = (n + (BLK - 1)) >> 7
        where = (((gy - s // 8) & 3) * 8 + ((gz - s % 8) & 7)) * PER
        inside = (k >= off) & (k < off + blocks)
        source = jnp.where(inside, where + ((k - off) >> 5), source)
        off = off + blocks
        every = every + n
    slots = (off - g + (NG - 1)) >> 5
    most = (off + (NG - 1)) >> 5
    more = (most > FIRST).astype(jnp.int32)
    filled = jnp.where(sub == 0, source, jnp.where(sub == 1, every, jnp.where(sub == 2, slots, more)))
    table[...] = filled
    tab[...] = filled
    pick_smem = pltpu.make_async_copy(tab, stab, own.at[0])
    pick_smem.start()

    second()
    third()
    pick_smem.wait()
    kind[0, 0] = stab[3, 0]

    def give_peak(i, slot):
        at = peaks.at[pl.ds(slot * 16, 16)]
        return over_view((v + i) % NV, top, at, s_peak.at[i], r_peak.at[slot])

    each(1, NV, lambda i: give_peak(i, v).start())
    peaks[pl.ds(v * 16, 16)] = top[...]
    keep.wait()
    each(1, NG, lambda i: pair(i).wait_recv())
    spread(
        out, FIRST, lambda q: stab[0, q], mine, s_own, r_own, s_side, r_side, s_far, r_far, lambda: None
    )
    each(1, NV, lambda i: give_peak(i, (v + i) % NV).wait_recv())
    each(1, NV, lambda i: give_peak(i, v).wait_send())
    each(1, NV, lambda i: give_best(i, (v + i) % NV).wait_recv())

    each(1, NG, lambda i: tell(i, g).wait_send())
    each(1, NG, lambda i: pair(i).wait_send())
    each(1, NV, lambda i: give_part(i, v).wait_send())
    each(1, NV, lambda i: give_pack(i, v).wait_send())
    each(1, NV, lambda i: give_best(i, v).wait_send())

    @pl.when(v > 0)
    def _():
        give_top(0).wait_send()

    each(1, 4, lambda t: give_top(t).wait_send())


def share_kernel(mine, table, out, *sems):
    v = lax.axis_index("view")
    barrier = pltpu.get_barrier_semaphore()
    each(1, NV, lambda i: pl.semaphore_signal(barrier, inc=1, device_id={"view": (v + i) % NV}, device_id_type=MESH))
    spread(out, CAP - FIRST, lambda q: table[0, FIRST + q], mine, *sems, lambda: pl.semaphore_wait(barrier, NV - 1))


def lay_kernel(more, table, best, peaks, tiles, *refs):
    rest, _, clones, peak, total, stage, sem = refs if more else (None, *refs)
    sub = lax.broadcasted_iota(jnp.int32, (8, 128), 0)
    used = table[2, 0]
    total[0, 0] = table[1, 0]

    def cols(at):
        return pl.ds(pl.multiple_of(at * BLK, BLK), BLK)

    def runs(count, most):
        for n in (64, 32, 16, 8, 4, 2, 1):
            if n <= most:
                yield (count & n) != 0, pl.multiple_of((count & (256 - 2 * n)) * BLK, BLK), n * BLK

    if more:
        pieces = [(tiles, 0, (True, 0, FIRST * BLK))]
        pieces += [(rest, FIRST, run) for run in runs(used - FIRST, CAP - FIRST)]
    else:
        pieces = [(tiles, 0, run) for run in runs(used, FIRST)]
    main, last = [], []
    for src, first, (on, at, size) in pieces:
        to = pl.multiple_of(at + first * BLK, BLK)
        main.append((on, pltpu.make_async_copy(
            src.at[0:56, pl.ds(at, size)], clones.at[0:56, pl.ds(to, size)], sem.at[0]
        )))
        last.append((on, pltpu.make_async_copy(
            stage.at[0 : ROWS - 56, pl.ds(to, size)], clones.at[56:ROWS, pl.ds(to, size)], sem.at[1]
        )))
    for on, copy in main:
        pl.when(on)(copy.start)

    def finish(src, first):
        def one(q):
            tops = peaks[table[0, q]]
            gtop = jnp.broadcast_to(jnp.sqrt(tops[0:1]), (8, 128))
            ltop = jnp.broadcast_to(3.0 * jnp.sqrt(tops[1:2]), (8, 128))
            tile = src[56:64, cols(q - first)]
            stage[:, cols(q)] = jnp.where(sub == 3, gtop, jnp.where(sub == 4, ltop, tile))

        return one

    each(jnp.int32(0), jnp.minimum(used, FIRST), finish(tiles, 0))
    if more:
        each(jnp.int32(FIRST), used, finish(rest, FIRST))
    for on, copy in last:
        pl.when(on)(copy.start)

    def roots(c, _):
        s = pl.ds(pl.multiple_of(c * 1024, 1024), 1024)
        piece, at = c // 2, pl.multiple_of((c % 2) * 8, 8)
        peak[0:1, s] = jnp.sqrt(best[piece, 0, pl.ds(at, 8), :]).reshape(1, 1024)
        peak[1:2, s] = (3.0 * jnp.sqrt(best[piece, 1, pl.ds(at, 8), :])).reshape(1, 1024)
        return 0

    lax.fori_loop(0, 16, roots, 0)
    for on, copy in main + last:
        pl.when(on)(copy.wait)


def body(means, scales, quats, attrs, grad_screen, visible, clone_mask, rotation, shift, focal):
    f32, i32 = jnp.float32, jnp.int32
    shape = jax.ShapeDtypeStruct
    dma = pltpu.SemaphoreType.DMA
    view_sems = [dma((2, CHUNKS))] * 2 + [dma((4, CHUNKS))] * 2 + [dma((CHUNKS,))] * 2
    mask = clone_mask.reshape(128, 128)
    part, packed, tiles, count, blank = pl.pallas_call(
        front_kernel,
        in_specs=[HBM] * 10,
        out_specs=(VMEM,) * 4 + (HBM,),
        out_shape=(
            shape((NV, 2, 16, 128), f32),
            shape((CAP, 2, 128), f32),
            shape((CAP, 8, 128), f32),
            shape((8, 128), i32),
            shape((ROWS, G), f32),
        ),
        scratch_shapes=[
            pltpu.VMEM((128, 128), i32),
            pltpu.VMEM((3, G), f32),
            pltpu.VMEM((3, G), f32),
            pltpu.VMEM((4, G), f32),
            pltpu.VMEM((4, 2, G), f32),
            pltpu.VMEM((4, G), i32),
            pltpu.SMEM((3, 4, 3), f32),
            pltpu.SMEM((4, 3), f32),
            pltpu.SMEM((4,), f32),
            pltpu.VMEM((8, G), f32),
            pltpu.VMEM((8, G), f32),
            pltpu.VMEM((8, G), f32),
            pltpu.VMEM((8, G), f32),
            pltpu.VMEM((128, 128), i32),
            pltpu.VMEM((8, 128), i32),
            pltpu.SMEM((8, 128), i32),
            pltpu.VMEM((8, G), f32),
            dma((3,)),
            dma((9,)),
            dma((NV,)),
        ],
        compiler_params=pltpu.CompilerParams(vmem_limit_bytes=16 * 2**20),
        name="front",
    )(
        *(
            pltpu.with_memory_space_constraint(a, pltpu.HBM)
            for a in (mask, means, scales, quats, grad_screen, visible, rotation.transpose(1, 0, 2), shift, focal, attrs)
        )
    )

    mine, out, peaks, best, _, table, kind = pl.pallas_call(
        move_kernel,
        in_specs=[VMEM] * 4,
        out_specs=(VMEM,) * 6 + (SMEM,),
        out_shape=(
            shape((CAP, 8, 128), f32),
            shape((8 * NV, FIRST * BLK), f32),
            shape((CAP, 2, 128), f32),
            shape((NV, 2, 16, 128), f32),
            shape((NG, 8, 128), i32),
            shape((8, 128), i32),
            shape((1, 1), i32),
        ),
        scratch_shapes=[
            pltpu.VMEM((NV, 2, 16, 128), f32),
            pltpu.VMEM((NV, 16, 2, 128), f32),
            pltpu.VMEM((2, 16, 128), f32),
            pltpu.VMEM((16, 2, 128), f32),
            pltpu.VMEM((16, 2, 128), f32),
            pltpu.VMEM((CAP, 8, 128), f32),
            pltpu.VMEM((CAP, 2, 128), f32),
            pltpu.VMEM((8, 128), i32),
            pltpu.SMEM((8, 128), i32),
        ]
        + [dma((NV,))] * 8
        + [dma((NG,))] * 4
        + [dma((4,))] * 2
        + view_sems
        + [dma((2,))],
        compiler_params=pltpu.CompilerParams(
            collective_id=0, has_side_effects=True, vmem_limit_bytes=16 * 2**20
        ),
        name="move",
    )(part, packed, tiles, count)

    share = pl.pallas_call(
        share_kernel,
        in_specs=[VMEM, SMEM],
        out_specs=VMEM,
        out_shape=shape((8 * NV, (CAP - FIRST) * BLK), f32),
        scratch_shapes=view_sems,
        compiler_params=pltpu.CompilerParams(
            collective_id=1, has_side_effects=True, vmem_limit_bytes=16 * 2**20
        ),
        name="share",
    )

    def lay(more, table, best, peaks, *tiles_and_blank):
        return pl.pallas_call(
            functools.partial(lay_kernel, more),
            in_specs=[SMEM, VMEM, VMEM] + [VMEM] * (1 + more) + [HBM],
            out_specs=(HBM, VMEM, SMEM),
            out_shape=(shape((ROWS, G), f32), shape((2, G), f32), shape((1, 1), i32)),
            input_output_aliases={4 + more: 0},
            scratch_shapes=[pltpu.VMEM((8, G), f32), dma((2,))],
            compiler_params=pltpu.CompilerParams(vmem_limit_bytes=16 * 2**20),
            name="lay_more" if more else "lay",
        )(table, best, peaks, *tiles_and_blank)

    def few(mine, table, best, peaks, out, blank):
        return lay(False, table, best, peaks, out, pltpu.with_memory_space_constraint(blank, pltpu.HBM))

    def many(mine, table, best, peaks, out, blank):
        rest = share(mine, table)
        return lay(True, table, best, peaks, out, rest, pltpu.with_memory_space_constraint(blank, pltpu.HBM))

    blank = pltpu.with_memory_space_constraint(blank, pltpu.HBM)
    clones, peak, total = lax.switch(kind.reshape(()), [few, many], mine, table, best, peaks, out, blank)
    return (peak, clones, total.reshape(()))


def solution(mesh):
    return jax.shard_map(
        body,
        mesh=mesh,
        in_specs=(
            P(None, "gauss"),
            P(None, "gauss"),
            P(None, "gauss"),
            P(None, "gauss"),
            P("view", None, "gauss"),
            P("view", "gauss"),
            P("gauss"),
            P("view", None, None),
            P("view", None),
            P("view"),
        ),
        out_specs=(P(None, "gauss"), P(None, "gauss"), P()),
        check_vma=False,
    )
```
